32 devices in a mesh: lat: 4 (over y, x), lon: 8 (over z, core).
Axes of the slice: x: 2, y: 2, z: 4, core: 2. Of those that a mesh axis runs over, the one named last changes fastest.
Arguments:
- field: float32 [64, 2048, 128], P('lat', 'lon'), may hold values from -6 to 6
- ocean: int32 [64, 2048], P('lat', 'lon'), may hold values 0 or 1
- modes: int32 [16], replicated, may hold values from 1 to 1023, as said below
- spectral_weight: float32 [16, 2, 128, 128], P('lon'), may hold values from -0.375 to 0.375
- local_weight: float32 [128, 128], replicated, may hold values from -0.5 to 0.5
- layer_bias: float32 [128], replicated, may hold values from -4 to 4
- conv_weight: float32 [3, 3, 128, 128], replicated, may hold values from -0.1875 to 0.1875
- conv_bias: float32 [128], replicated, may hold values from -2 to 2
Outputs:
- decoded: float32 [64, 2048, 128], P('lat', 'lon')
The draws below stay inside these ranges and needn't reach their ends.
Inputs may be any that keep to these rules, and one draw needn't show every extreme that they name: `modes`: distinct wavenumbers.
All inputs are finite; a program needn't handle non-finite values. No bound on the sum of `ocean` on one device may be relied on, other than what follows from the above.
Results may differ from the reference program's by a relative error of at most 0.0001.
Values sent between devices are 32-bit elements; how exact they have to be, the bound alone decides.
No kernel may reach another device: no remote copies, remote signals or barrier semaphores. Data moves between devices by JAX's collectives and lax.ppermute only.
A program may use at most 64 MiB of HBM per device.

```python
import math
import jax
import jax.numpy as jnp
from jax import lax

C = 128
NLAT = 64
NLON = 2048
MODES = 16


def draw_modes(key, part):
    return (jax.random.permutation(key, NLON // 2 - 1)[:MODES] + 1).astype(jnp.int32)


def with_ends(array, key, least, top_value):
    extent = array.shape
    spot = [jax.random.randint(jax.random.fold_in(key, axis), (), 0, extent[axis]) for axis in range(len(extent))]
    array = array.at[tuple(spot)].set(least)
    longest = extent.index(max(extent))
    spot[longest] = (spot[longest] + 1) % extent[longest]
    return array.at[tuple(spot)].set(top_value)


def level_of(key, extent, cuts, low, largest):
    def one(position, blocks):
        draws = jax.random.uniform(jax.random.fold_in(jax.random.fold_in(key, 6), position), (blocks,), jnp.float32, low / len(cuts), largest / len(cuts))
        return jnp.repeat(jnp.exp(draws), extent[position] // blocks).reshape((-1,) + (1,) * (len(extent) - position - 1))

    level = one(*cuts[0])
    for cut in cuts[1:]:
        level = level * one(*cut)
    return level


def noise(rng, extent, spread, limit, cuts=(), kind=jnp.bfloat16):
    loudness = level_of(rng, extent, cuts, -0.22, 0.18) if cuts else 1.0
    result = jax.random.normal(rng, extent, jnp.float32) * spread * loudness
    return jnp.minimum(jnp.maximum(result, -limit), limit).astype(kind)


def setup_inputs(seed: int = 0) -> dict:
    arg_keys = jax.random.split(jax.random.key(seed), 9)
    field = noise(arg_keys[0], (NLAT, NLON, C), 1.0, 6.0, ((0, 4), (1, 8)), jnp.float32)
    ocean = with_ends((jax.random.randint(arg_keys[1], (NLAT, NLON), 0, 3) < 2).astype(jnp.int32), jax.random.fold_in(arg_keys[1], 1), 0, 1)
    modes = draw_modes(jax.random.fold_in(arg_keys[8], 71), 0)
    spectral_weight = noise(arg_keys[3], (MODES, 2, C, C), (2 * C) ** -0.5, 0.375, ((0, 8),), jnp.float32)
    local_weight = noise(arg_keys[4], (C, C), C ** -0.5, 0.5, (), jnp.float32)
    layer_bias = noise(arg_keys[5], (C,), 1.0, 4.0, (), jnp.float32)
    conv_weight = noise(arg_keys[6], (3, 3, C, C), (9 * C) ** -0.5, 0.1875, (), jnp.float32)
    conv_bias = noise(arg_keys[7], (C,), 0.5, 2.0, (), jnp.float32)
    return dict(field=field, ocean=ocean, modes=modes, spectral_weight=spectral_weight, local_weight=local_weight, layer_bias=layer_bias, conv_weight=conv_weight, conv_bias=conv_bias)


HIGH = lax.Precision.HIGHEST

def reference(field, ocean, modes, spectral_weight, local_weight, layer_bias, conv_weight, conv_bias):
    lon_ids = jnp.arange(NLON, dtype=jnp.int32)
    product = modes[:, None] * lon_ids[None, :] % NLON
    theta = product.astype(jnp.float32) * (2.0 * math.pi / NLON)
    cosine = jnp.cos(theta)
    sine = jnp.sin(theta)
    real_part = jnp.einsum('mj,ijc->mic', cosine, field, precision=HIGH) / math.sqrt(NLON)
    imag_part = -jnp.einsum('mj,ijc->mic', sine, field, precision=HIGH) / math.sqrt(NLON)
    coeffs = jnp.concatenate([real_part, imag_part], -1)
    w_real = spectral_weight[:, 0]
    w_imag = spectral_weight[:, 1]
    upper = jnp.concatenate([w_real, w_imag], -1)
    lower = jnp.concatenate([-w_imag, w_real], -1)
    blocks = jnp.concatenate([upper, lower], 1)
    mixed = jnp.einsum('mic,mcd->mid', coeffs, blocks, precision=HIGH)
    spectral = jnp.einsum('mj,mic->ijc', cosine, mixed[:, :, :C], precision=HIGH)
    spectral = spectral - jnp.einsum('mj,mic->ijc', sine, mixed[:, :, C:], precision=HIGH)
    spectral = spectral * (2.0 / math.sqrt(MODES))
    wet = ocean.astype(jnp.float32)[:, :, None]
    local = jnp.einsum('ijc,cd->ijd', field, local_weight, precision=HIGH)
    hidden = wet * jax.nn.gelu(spectral + local + layer_bias, approximate=True)
    padded = jnp.concatenate([hidden[:, -1:], hidden, hidden[:, :1]], 1)
    padded = jnp.pad(padded, ((1, 1), (0, 0), (0, 0)))

    def one_row(index):
        block = lax.dynamic_slice_in_dim(padded, index, 3, 0)
        total = jnp.zeros((NLON, C), jnp.float32)
        for row_tap in range(3):
            for col_tap in range(3):
                total = total + jnp.dot(block[row_tap, col_tap:col_tap + NLON], conv_weight[row_tap, col_tap], precision=HIGH)
        return total
    conv = lax.map(one_row, jnp.arange(NLAT, dtype=jnp.int32))
    return wet * (conv + conv_bias)
```

```python
import math

import jax
import jax.numpy as jnp
from jax import lax
from jax.sharding import PartitionSpec as P

HIGH = lax.Precision.HIGH


def flip_of(distance, chips):
    return 1 if distance in (1, chips - 1) else 0


def chip_moves(distance, chips, flip):
    return [
        (2 * chip + core, 2 * ((chip + distance) % chips) + (core ^ flip))
        for chip in range(chips)
        for core in range(2)
    ]


def pair_moves(chips):
    return [(device, device ^ 1) for device in range(2 * chips)]


def distances(chips):
    far = [d for d in range(2, chips - 1)]
    return far + [1, chips - 1]


def tables(mode_ids, lon_start, width, total_lon):
    lon_ids = lon_start + jnp.arange(width, dtype=jnp.int32)
    lon_ids = (lon_ids + total_lon) % total_lon
    product = mode_ids[:, None] * lon_ids[None, :] % total_lon
    theta = product.astype(jnp.float32) * (2.0 * math.pi / total_lon)
    return (jnp.cos(theta), jnp.sin(theta))


def mode_order(modes, owners, per_device):
    ids = (owners[:, None] * per_device + jnp.arange(per_device)).reshape(-1)
    hit = ids[:, None] == jnp.arange(modes.shape[0])[None, :]
    return jnp.sum(jnp.where(hit, modes[None, :], 0), axis=1)


def mix_modes(coeffs, weights):
    w_real = weights[:, 0]
    w_imag = weights[:, 1]
    upper = jnp.concatenate([w_real, w_imag], -1)
    lower = jnp.concatenate([-w_imag, w_real], -1)
    blocks = jnp.concatenate([upper, lower], 1)
    return jnp.einsum("mic,mcd->mid", coeffs, blocks, precision=HIGH)


def per_device(
    field, ocean, modes, spectral_weight, local_weight, layer_bias, conv_weight, conv_bias
):
    rows, width, channels = field.shape
    devices = lax.axis_size("lon")
    chips = devices // 2
    bands = lax.axis_size("lat")
    here = lax.axis_index("lon")
    chip, core = here // 2, here % 2
    total_lon = width * devices
    per = modes.shape[0] // devices
    lon_start = here * width
    steps = distances(chips)
    flips = [flip_of(d, chips) for d in range(chips)]

    dist = jnp.arange(chips)
    flip = (dist == 1) | (dist == chips - 1)
    keep_owner = 2 * ((chip + dist) % chips) + (core ^ flip.astype(jnp.int32))
    give_owner = keep_owner ^ 1
    out_modes = mode_order(modes, jnp.concatenate([keep_owner, give_owner]), per)
    cosine, sine = tables(out_modes, lon_start, width, total_lon)
    trig = jnp.stack([cosine, -sine]) / math.sqrt(total_lon)
    coeffs = jnp.einsum("tmj,ijc->mitc", trig, field, precision=HIGH)
    coeffs = coeffs.reshape(2, chips, per, rows, 2 * channels)

    wet = ocean.astype(jnp.float32)

    def packet(col):
        land = jnp.broadcast_to(wet[:, col][:, None], (rows, channels))
        return jnp.concatenate([field[:, col], land], -1)[None]

    first, last = packet(0), packet(width - 1)
    near = jnp.where(core == 0, last, first)
    away = jnp.where(core == 0, first, last)

    give = coeffs[1].reshape(chips * per, rows, 2 * channels)
    got = lax.ppermute(jnp.concatenate([give, near]), "lon", pair_moves(chips))
    near_in = got[-1]
    summed = coeffs[0] + got[:-1].reshape(coeffs[0].shape)
    own = summed[0]
    far_in = {}
    for d in steps:
        send = summed[d]
        if flips[d]:
            send = jnp.concatenate([send, away])
        part = lax.ppermute(send, "lon", chip_moves(d, chips, flips[d]))
        if flips[d]:
            far_in[d] = part[-1]
            part = part[:-1]
        own = own + part
    left = jnp.where(core == 0, far_in[1], near_in)
    right = jnp.where(core == 0, near_in, far_in[chips - 1])

    own_mixed = mix_modes(own, spectral_weight)
    parts = [own_mixed]
    for d in steps:
        parts.append(lax.ppermute(own_mixed, "lon", chip_moves(d, chips, 0)))
    parts = jnp.stack(parts)
    other = lax.ppermute(parts, "lon", pair_moves(chips))
    mixed = jnp.stack([parts, other]).reshape(modes.shape[0], rows, 2, channels)
    source_chip = jnp.stack([(chip - d) % chips for d in [0] + steps])
    owners = jnp.concatenate([2 * source_chip + core, 2 * source_chip + (1 - core)])
    in_modes = mode_order(modes, owners, per)
    cosine, sine = tables(in_modes, lon_start - 1, width + 2, total_lon)
    trig = jnp.stack([cosine, -sine]) * (2.0 / math.sqrt(modes.shape[0]))

    wide = jnp.concatenate([left[:, None, :channels], field, right[:, None, :channels]], 1)
    wet_wide = jnp.concatenate([left[:, channels:channels + 1], wet, right[:, channels:channels + 1]], 1)
    spectral = jnp.einsum("tmj,mitc->ijc", trig, mixed, precision=HIGH)
    local = jnp.einsum("ijc,cd->ijd", wide, local_weight, precision=HIGH)
    hidden = wet_wide[:, :, None] * jax.nn.gelu(spectral + local + layer_bias, approximate=True)

    up = [(i, i + 1) for i in range(bands - 1)]
    down = [(i + 1, i) for i in range(bands - 1)]
    above = lax.ppermute(hidden[-1:], "lat", up)
    below = lax.ppermute(hidden[:1], "lat", down)
    padded = jnp.concatenate([above, hidden, below])
    conv = jnp.zeros((rows, width, channels), jnp.float32)
    for row_tap in range(3):
        for col_tap in range(3):
            window = padded[row_tap : row_tap + rows, col_tap : col_tap + width]
            conv = conv + jnp.einsum(
                "ijc,cd->ijd", window, conv_weight[row_tap, col_tap], precision=HIGH
            )
    return wet[:, :, None] * (conv + conv_bias)


def solution(mesh):
    in_specs = (
        P("lat", "lon", None),
        P("lat", "lon"),
        P(),
        P("lon", None, None, None),
        P(),
        P(),
        P(),
        P(),
    )
    out_specs = P("lat", "lon", None)
    return jax.shard_map(
        per_device, mesh=mesh, in_specs=in_specs, out_specs=out_specs, check_vma=False
    )
```

```python
import functools
import math

import jax
import jax.numpy as jnp
from jax import lax
from jax.experimental import pallas as pl
from jax.experimental.pallas import tpu as pltpu
from jax.sharding import PartitionSpec as P

LANES = 128
TAIL = 16
MIB = 1 << 20
F32 = jnp.float32
BF16 = jnp.bfloat16


def flip_of(distance, chips):
    return 1 if distance in (1, chips - 1) else 0


def chip_moves(distance, chips, flip):
    return [
        (2 * chip + core, 2 * ((chip + distance) % chips) + (core ^ flip))
        for chip in range(chips)
        for core in range(2)
    ]


def pair_moves(chips):
    return [(device, device ^ 1) for device in range(2 * chips)]


def distances(chips):
    return [1, chips - 1] + list(range(2, chips - 1))


def split(x):
    high = x.astype(BF16)
    return high, (x - high.astype(F32)).astype(BF16)


def dot(a, b):
    return lax.dot_general(a, b, (((1,), (0,)), ((), ())), preferred_element_type=F32)


def fill(blocks, depth):
    missing = depth - sum(block.shape[0] for block in blocks)
    if missing:
        blocks = blocks + [jnp.zeros((missing,) + blocks[0].shape[1:], blocks[0].dtype)]
    return jnp.concatenate(blocks, 0)


def angles(mode_list, lon, total_lon):
    row = lax.broadcasted_iota(jnp.int32, lon.shape, 0)
    ids = jnp.zeros(lon.shape, jnp.int32)
    for index, mode in enumerate(mode_list):
        ids = jnp.where(row == index, mode, ids)
    product = ids * lon
    if total_lon & (total_lon - 1):
        product = lax.rem(product, total_lon)
    else:
        product = product & (total_lon - 1)
    return product.astype(F32) * (2.0 * math.pi / total_lon)


def forward_kernel(
    chips, per, total_lon, where_ref, modes_hbm, field_hbm, ocean_hbm, give_ref, keep_ref, away_ref,
    modes_ref, field_ref, ocean_ref, small_sem, field_sem,
):
    rows, width, channels = field_ref.shape
    chunks = field_sem.shape[0]
    step = rows // chunks
    first_copy = pltpu.make_async_copy(modes_hbm, modes_ref, small_sem.at[0])
    first_copy.start()
    copies = []
    for k in range(chunks):
        part = pl.ds(k * step, step)
        copies.append(pltpu.make_async_copy(field_hbm.at[part], field_ref.at[part], field_sem.at[k]))
        copies[-1].start()
    ocean_copy = pltpu.make_async_copy(ocean_hbm, ocean_ref, small_sem.at[1])
    ocean_copy.start()
    here = where_ref[0]
    chip, core = here // 2, lax.rem(here, 2)
    first_copy.wait()
    mode_list = []
    for flipped in range(2):
        for d in range(chips):
            owner = 2 * lax.rem(chip + d, chips)
            owner = owner + lax.rem(core + flipped + flip_of(d, chips), 2)
            mode_list += [modes_ref[owner * per + t] for t in range(per)]
    count = len(mode_list)
    half = count // 2
    lon = here * width + lax.broadcasted_iota(jnp.int32, (count, width), 1)
    theta = angles(mode_list, lon, total_lon)
    scale = 1.0 / math.sqrt(total_lon)
    table = jnp.concatenate([jnp.cos(theta) * scale, -jnp.sin(theta) * scale], 0)
    lhs = jnp.concatenate(split(table), 0)
    for i in range(rows):
        if i % step == 0:
            copies[i // step].wait()
        rhs = jnp.concatenate(split(field_ref[i]), 1)
        product = dot(lhs, rhs)
        total = product[: 2 * count] + product[2 * count :]
        total = total[:, :channels] + total[:, channels:]
        keep_ref[:half, i, :channels] = total[:half]
        give_ref[:half, i, :channels] = total[half:count]
        keep_ref[:half, i, channels:] = total[count : count + half]
        give_ref[:half, i, channels:] = total[count + half :]
    ocean_copy.wait()
    last = field_ref[:, width - 1, :]
    first = field_ref[:, 0, :]
    land = ocean_ref[...].astype(F32)
    last_wet = jnp.broadcast_to(land[:, width - 1 : width], (rows, channels))
    first_wet = jnp.broadcast_to(land[:, :1], (rows, channels))
    near_is_last = core == 0
    give_ref[half, :, :channels] = jnp.where(near_is_last, last, first)
    give_ref[half, :, channels:] = jnp.where(near_is_last, last_wet, first_wet)
    away_ref[0, :, :channels] = jnp.where(near_is_last, first, last)
    away_ref[0, :, channels:] = jnp.where(near_is_last, first_wet, last_wet)


def prepare_kernel(
    chips, per, total_lon, width, where_ref, modes_ref, local_ref, conv_ref, spectral_ref,
    trig_ref, local_out, w1_ref, w2_ref, w3_ref, mix_ref,
):
    channels = local_ref.shape[0]
    wide = 2 * channels
    for t in range(per):
        real, imag = spectral_ref[t, 0], spectral_ref[t, 1]
        top = jnp.concatenate(split(jnp.concatenate([real, imag], 1)), 1)
        low = jnp.concatenate(split(jnp.concatenate([-imag, real], 1)), 1)
        mix_ref[t * wide : t * wide + channels, :] = top
        mix_ref[t * wide + channels : (t + 1) * wide, :] = low
    here = where_ref[0]
    chip, core = here // 2, lax.rem(here, 2)
    mode_list = []
    for flipped in range(2):
        for d in [0] + distances(chips):
            source = 2 * lax.rem(chip - d + chips, chips) + lax.rem(core + flipped, 2)
            mode_list += [modes_ref[source * per + t] for t in range(per)]
    count = len(mode_list)
    block = width + TAIL
    padded = -(-block // LANES) * LANES
    place = lax.broadcasted_iota(jnp.int32, (count, padded), 1)
    place = jnp.where(place == block - 1, -1, place)
    lon = here * width + place + total_lon
    lon = jnp.where(lon >= total_lon, lon - total_lon, lon)
    lon = jnp.where(lon >= total_lon, lon - total_lon, lon)
    theta = angles(mode_list, lon, total_lon)
    scale = 2.0 / math.sqrt(count)
    table = jnp.concatenate([jnp.cos(theta) * scale, -jnp.sin(theta) * scale], 0)
    high, low = split(table)
    high, low = high.astype(F32), low.astype(F32)
    depth = trig_ref.shape[1]
    stacked = fill([high, low, high], depth)
    trig_ref[...] = stacked.T[:block].astype(BF16)
    local_out[...] = jnp.concatenate(split(local_ref[...]), 1)
    for col in range(3):
        left = slice(col * channels, (col + 1) * channels)
        right = slice((3 + col) * channels, (4 + col) * channels)
        for row in range(2):
            at = slice(row * channels, (row + 1) * channels)
            top, bottom = split(conv_ref[row, col])
            w1_ref[at, left] = top
            w1_ref[at, right] = bottom
            w3_ref[at, left] = top
        top, bottom = split(conv_ref[2, col])
        w2_ref[:channels, left] = top
        w2_ref[:channels, right] = bottom
        w2_ref[channels:, left] = top
        w2_ref[channels:, right] = jnp.zeros_like(top)


def gelu(x):
    inner = math.sqrt(2.0 / math.pi) * (x + 0.044715 * (x * x * x))
    return x * (0.5 * (1.0 + jnp.tanh(inner)))


def mix_kernel(per, rows, *refs):
    summed_ref, *part_refs, mix_ref, out_ref = refs
    wide = summed_ref.shape[1]
    for t in range(per):
        at = slice(t * rows, (t + 1) * rows)
        total = summed_ref[at, :]
        for part in part_refs:
            total = total + part[at, :]
        high, low = split(total)
        weights = mix_ref[t * wide : (t + 1) * wide, :]
        y = dot(high, weights)
        out_ref[at, :] = y[:, :wide] + y[:, wide:] + dot(low, weights[:, :wide])


def hidden_kernel(
    per, where_ref, field_ref, got_ref, west_ref, east_ref, ocean_ref, mixed_ref, trig_ref, local_ref, bias_ref,
    high_ref, low_ref, edge_ref,
):
    rows, width, channels = field_ref.shape
    block = width + TAIL
    depth = trig_ref.shape[1]
    wet = ocean_ref[...].astype(F32).T
    empty = jnp.zeros((depth, channels), BF16)
    trig = trig_ref[...]
    local = local_ref[...]
    south = lax.rem(where_ref[0], 2) == 0
    even = lax.rem(where_ref[1], 2)
    near = got_ref[got_ref.shape[0] - rows :, :]
    left = jnp.where(south, west_ref[per * rows :, :], near)
    right = jnp.where(south, near, east_ref[per * rows :, :])
    place = lax.broadcasted_iota(jnp.int32, (TAIL, 2 * channels), 0)
    for i in range(rows):
        tail = jnp.where(place == TAIL - 1, left[i : i + 1], jnp.where(place == 0, right[i : i + 1], 0.0))
        x = jnp.concatenate([field_ref[i], tail[:, :channels]], 0)
        x_high, x_low = split(x)
        mixed = jnp.concatenate([mixed_ref[:, i, :channels], mixed_ref[:, i, channels:]], 0)
        m_high, m_low = split(mixed)
        lower = fill([m_high, m_high, m_low], depth)
        rhs = jnp.concatenate([local, jnp.concatenate([lower, empty], 1)], 0)
        lhs = jnp.concatenate([x_high, trig], 1)
        y = dot(lhs, rhs)
        y = y[:, :channels] + y[:, channels:] + dot(x_low, local[:, :channels])
        y = gelu(y + bias_ref[...])
        mask = jnp.concatenate(
            [jnp.broadcast_to(wet[:, i : i + 1], (width, channels)), tail[:, channels:]], 0
        )
        y = y * mask
        h_high, h_low = split(y)
        high_ref[i * block : (i + 1) * block, :] = h_high
        low_ref[i * block : (i + 1) * block, :] = h_low
        if i == 0:
            edge_ref[1 - even] = y
        if i == rows - 1:
            edge_ref[even] = y


def conv_rows(a1, a2, a3, w1, w2, w3, channels, block, count):
    n = 3 * channels
    y = dot(a1, w1) + dot(a2, w2)
    z = y[:, :n] + y[:, n:] + dot(a3, w3)
    out = []
    for r in range(count):
        t = z[r * block : (r + 1) * block]
        west = pltpu.roll(t[:, :channels], 1, 0)
        east = pltpu.roll(t[:, 2 * channels :], block - 1, 0)
        out.append((west + t[:, channels : 2 * channels] + east)[: block - TAIL])
    return out


def inner_kernel(high_ref, low_ref, ocean_ref, bias_ref, w1_ref, w2_ref, w3_ref, out_ref, buf_ref, wet_ref, sem_ref):
    rows, width = ocean_ref.shape
    channels = high_ref.shape[1]
    block = width + TAIL
    wet = ocean_ref[...].astype(F32).T
    for g in range((rows - 2) // 2):
        i = 1 + 2 * g

        def at(ref, first):
            return ref[first * block : (first + 2) * block, :]

        a1 = jnp.concatenate([at(high_ref, i - 1), at(high_ref, i)], 1)
        a2 = jnp.concatenate([at(high_ref, i + 1), at(low_ref, i + 1)], 1)
        a3 = jnp.concatenate([at(low_ref, i - 1), at(low_ref, i)], 1)
        res = conv_rows(a1, a2, a3, w1_ref[...], w2_ref[...], w3_ref[...], channels, block, 2)
        for r in range(2):
            buf_ref[2 * g + r] = (res[r] + bias_ref[...]) * wet[:, i + r : i + r + 1]
        pltpu.make_async_copy(buf_ref.at[pl.ds(2 * g, 2)], out_ref.at[pl.ds(i, 2)], sem_ref.at[g]).start()
    for g in range((rows - 2) // 2):
        pltpu.make_async_copy(buf_ref.at[pl.ds(2 * g, 2)], out_ref.at[pl.ds(1 + 2 * g, 2)], sem_ref.at[g]).wait()


def outer_kernel(
    where_ref, high_ref, low_ref, first_ref, second_ref, ocean_ref, bias_ref, w1_ref, w2_ref, w3_ref, in_ref, out_ref, buf_ref, sem_ref
):
    rows, width = ocean_ref.shape
    channels = high_ref.shape[1]
    block = width + TAIL
    wet = ocean_ref[...].astype(F32).T

    def at(ref, row):
        return ref[row * block : (row + 1) * block, :]

    even = lax.rem(where_ref[1], 2) == 0
    up_high, up_low = split(jnp.where(even, second_ref[0], first_ref[0]))
    down_high, down_low = split(jnp.where(even, first_ref[0], second_ref[0]))
    top = [(up_high, up_low)] + [(at(high_ref, r), at(low_ref, r)) for r in (0, 1)]
    bottom = [(at(high_ref, r), at(low_ref, r)) for r in (rows - 2, rows - 1)] + [(down_high, down_low)]

    def stack(k, part):
        return jnp.concatenate([top[k][part], bottom[k][part]], 0)

    a1 = jnp.concatenate([stack(0, 0), stack(1, 0)], 1)
    a2 = jnp.concatenate([stack(2, 0), stack(2, 1)], 1)
    a3 = jnp.concatenate([stack(0, 1), stack(1, 1)], 1)
    res = conv_rows(a1, a2, a3, w1_ref[...], w2_ref[...], w3_ref[...], channels, block, 2)
    copies = []
    for r, row in enumerate((0, rows - 1)):
        buf_ref[r] = (res[r] + bias_ref[...]) * wet[:, row : row + 1]
        copy = pltpu.make_async_copy(buf_ref.at[pl.ds(r, 1)], out_ref.at[pl.ds(row, 1)], sem_ref.at[r])
        copy.start()
        copies.append(copy)
    for copy in copies:
        copy.wait()


def vmem():
    return pl.BlockSpec(memory_space=pltpu.VMEM)


def smem():
    return pl.BlockSpec(memory_space=pltpu.SMEM)


def struct(shape, dtype=F32):
    return jax.ShapeDtypeStruct(shape, dtype)


def params(mib):
    return pltpu.CompilerParams(vmem_limit_bytes=mib * MIB)


def per_device(
    field, ocean, modes, spectral_weight, local_weight, layer_bias, conv_weight, conv_bias
):
    rows, width, channels = field.shape
    devices = lax.axis_size("lon")
    chips = devices // 2
    bands = lax.axis_size("lat")
    where = jnp.stack([lax.axis_index("lon"), lax.axis_index("lat")]).astype(jnp.int32)
    total_lon = width * devices
    total_modes = modes.shape[0]
    per = total_modes // devices
    half = chips * per
    block = width + TAIL
    steps = distances(chips)
    wide = 2 * channels
    chunks = 4

    give, keep, away = pl.pallas_call(
        functools.partial(forward_kernel, chips, per, total_lon),
        out_shape=(
            struct((half + 1, rows, wide)),
            struct((half, rows, wide)),
            struct((1, rows, wide)),
        ),
        in_specs=[smem()] + [pl.BlockSpec(memory_space=pltpu.MemorySpace.HBM)] * 3,
        out_specs=(vmem(), vmem(), vmem()),
        scratch_shapes=[
            pltpu.SMEM((total_modes,), jnp.int32),
            pltpu.VMEM((rows, width, channels), F32),
            pltpu.VMEM((rows, width), jnp.int32),
            pltpu.SemaphoreType.DMA((2,)),
            pltpu.SemaphoreType.DMA((chunks,)),
        ],
        compiler_params=params(16),
        name="forward",
    )(where, *[pltpu.with_memory_space_constraint(x, pltpu.MemorySpace.HBM) for x in (modes, field, ocean)])
    give = give.reshape((half + 1) * rows, wide)
    keep = keep.reshape(half * rows, wide)
    away = away.reshape(rows, wide)

    depth = -(-6 * total_modes // LANES) * LANES
    trig, local, w1, w2, w3, mix = pl.pallas_call(
        functools.partial(prepare_kernel, chips, per, total_lon, width),
        out_shape=(
            struct((block, depth), BF16),
            struct((channels, 2 * channels), BF16),
            struct((2 * channels, 6 * channels), BF16),
            struct((2 * channels, 6 * channels), BF16),
            struct((2 * channels, 3 * channels), BF16),
            struct((per * wide, 2 * wide), BF16),
        ),
        in_specs=[smem(), smem(), vmem(), vmem(), vmem()],
        out_specs=(vmem(),) * 6,
        compiler_params=params(16),
        name="prepare",
    )(where, modes, local_weight, conv_weight, spectral_weight)

    got = lax.ppermute(give, "lon", pair_moves(chips))
    summed = keep + got[: half * rows]
    size = per * rows
    parts = {}
    for d in steps:
        send = summed[d * size : (d + 1) * size]
        flip = flip_of(d, chips)
        if flip:
            send = jnp.concatenate([send, away])
        parts[d] = lax.ppermute(send, "lon", chip_moves(d, chips, flip))

    own_mixed = pl.pallas_call(
        functools.partial(mix_kernel, per, rows),
        out_shape=struct((size, wide)),
        in_specs=[vmem()] * (len(steps) + 2),
        out_specs=vmem(),
        compiler_params=params(8),
        name="mix",
    )(summed, *[parts[d] for d in steps], mix)
    gathered = [own_mixed]
    for d in steps:
        gathered.append(lax.ppermute(own_mixed, "lon", chip_moves(d, chips, 0)))
    gathered = jnp.concatenate(gathered)
    other = lax.ppermute(gathered, "lon", pair_moves(chips))
    mixed = jnp.concatenate([gathered, other]).reshape(total_modes, rows, wide)

    high, low, edge = pl.pallas_call(
        functools.partial(hidden_kernel, per),
        out_shape=(
            struct((rows * block, channels), BF16),
            struct((rows * block, channels), BF16),
            struct((2, block, channels)),
        ),
        in_specs=[smem()] + [vmem()] * 9,
        out_specs=(vmem(),) * 3,
        compiler_params=params(24),
        name="hidden",
    )(where, field, got, parts[1], parts[chips - 1], ocean, mixed, trig, local, layer_bias.reshape(1, channels))

    evens = [(i, i + 1) for i in range(0, bands - 1, 2)]
    odds = [(i, i + 1) for i in range(1, bands - 1, 2)]
    first = lax.ppermute(edge[:1], "lat", evens + [(b, a) for a, b in evens])
    second = lax.ppermute(edge[1:], "lat", odds + [(b, a) for a, b in odds])
    bias = conv_bias.reshape(1, channels)
    flops = 2 * 9 * 3 * rows * width * channels * channels
    inner = pl.pallas_call(
        inner_kernel,
        out_shape=struct((rows, width, channels)),
        in_specs=[vmem()] * 7,
        out_specs=pl.BlockSpec(memory_space=pl.ANY),
        scratch_shapes=[
            pltpu.VMEM((rows - 2, width, channels), F32),
            pltpu.VMEM((rows, width), F32),
            pltpu.SemaphoreType.DMA(((rows - 2) // 2,)),
        ],
        compiler_params=params(32),
        cost_estimate=pl.CostEstimate(flops=flops, transcendentals=0, bytes_accessed=4 * field.size),
        name="inner",
    )(high, low, ocean, bias, w1, w2, w3)
    return pl.pallas_call(
        outer_kernel,
        out_shape=struct((rows, width, channels)),
        in_specs=[smem()] + [vmem()] * 9 + [pl.BlockSpec(memory_space=pl.ANY)],
        out_specs=pl.BlockSpec(memory_space=pl.ANY),
        scratch_shapes=[
            pltpu.VMEM((2, width, channels), F32),
            pltpu.SemaphoreType.DMA((2,)),
        ],
        input_output_aliases={10: 0},
        compiler_params=params(32),
        name="outer",
    )(where, high, low, first, second, ocean, bias, w1, w2, w3, inner)


def solution(mesh):
    in_specs = (
        P("lat", "lon", None),
        P("lat", "lon"),
        P(),
        P("lon", None, None, None),
        P(),
        P(),
        P(),
        P(),
    )
    out_specs = P("lat", "lon", None)
    return jax.shard_map(
        per_device, mesh=mesh, in_specs=in_specs, out_specs=out_specs, check_vma=False
    )
```

```python
import functools
import math

import jax
import jax.numpy as jnp
from jax import lax
from jax.experimental import pallas as pl
from jax.experimental.pallas import tpu as pltpu
from jax.sharding import PartitionSpec as P

LANES = 128
TAIL = 16
MIB = 1 << 20
DRY = -(2.0**36)
F32 = jnp.float32
BF16 = jnp.bfloat16


def flip_of(distance, chips):
    return 1 if distance in (1, chips - 1) else 0


def chip_moves(distance, chips, flip):
    return [
        (2 * chip + core, 2 * ((chip + distance) % chips) + (core ^ flip))
        for chip in range(chips)
        for core in range(2)
    ]


def pair_moves(chips):
    return [(device, device ^ 1) for device in range(2 * chips)]


def distances(chips):
    return [1, chips - 1] + list(range(2, chips - 1))


def gather_source(chip, distance, chips):
    if chips & (chips - 1):
        return lax.rem(chip - distance + chips, chips)
    return chip ^ distance


def gather_moves(distance, chips):
    if chips & (chips - 1):
        return chip_moves(distance, chips, 0)
    return [
        (2 * chip + core, 2 * (chip ^ distance) + core) for chip in range(chips) for core in range(2)
    ]


def split(x):
    high = x.astype(BF16)
    return high, (x - high.astype(F32)).astype(BF16)


def dot(a, b):
    return lax.dot_general(a, b, (((1,), (0,)), ((), ())), preferred_element_type=F32)


def fill(blocks, depth):
    missing = depth - sum(block.shape[0] for block in blocks)
    if missing:
        blocks = blocks + [jnp.zeros((missing,) + blocks[0].shape[1:], blocks[0].dtype)]
    return jnp.concatenate(blocks, 0)


def angles(mode_list, lon, total_lon):
    row = lax.broadcasted_iota(jnp.int32, lon.shape, 0)
    ids = jnp.zeros(lon.shape, jnp.int32)
    for index, mode in enumerate(mode_list):
        ids = jnp.where(row == index, mode, ids)
    product = ids * lon
    if total_lon & (total_lon - 1):
        product = lax.rem(product, total_lon)
    else:
        product = product & (total_lon - 1)
    return product.astype(F32) * (2.0 * math.pi / total_lon)


def forward_kernel(
    chips, per, total_lon, modes_hbm, field_hbm, ocean_hbm, give_ref, keep_ref, away_ref,
    modes_ref, field_ref, ocean_ref, small_sem, field_sem,
):
    rows, width, channels = field_ref.shape
    chunks = field_sem.shape[0]
    step = rows // chunks
    first_copy = pltpu.make_async_copy(modes_hbm, modes_ref, small_sem.at[0])
    first_copy.start()
    copies = []
    for k in range(chunks):
        part = pl.ds(k * step, step)
        copies.append(pltpu.make_async_copy(field_hbm.at[part], field_ref.at[part], field_sem.at[k]))
        copies[-1].start()
    ocean_copy = pltpu.make_async_copy(ocean_hbm, ocean_ref, small_sem.at[1])
    ocean_copy.start()
    here = lax.axis_index("lon")
    chip, core = here // 2, lax.rem(here, 2)
    first_copy.wait()
    mode_list = []
    for flipped in range(2):
        for d in range(chips):
            owner = 2 * lax.rem(chip + d, chips)
            owner = owner + lax.rem(core + flipped + flip_of(d, chips), 2)
            mode_list += [modes_ref[owner * per + t] for t in range(per)]
    count = len(mode_list)
    half = count // 2
    lon = here * width + lax.broadcasted_iota(jnp.int32, (count, width), 1)
    theta = angles(mode_list, lon, total_lon)
    scale = 1.0 / math.sqrt(total_lon)
    table = jnp.concatenate([jnp.cos(theta) * scale, -jnp.sin(theta) * scale], 0)
    lhs = jnp.concatenate(split(table), 0)
    for i in range(rows):
        if i % step == 0:
            copies[i // step].wait()
        rhs = jnp.concatenate(split(field_ref[i]), 1)
        product = dot(lhs, rhs)
        total = product[: 2 * count] + product[2 * count :]
        total = total[:, :channels] + total[:, channels:]
        keep_ref[:half, i, :channels] = total[:half]
        give_ref[:half, i, :channels] = total[half:count]
        keep_ref[:half, i, channels:] = total[count : count + half]
        give_ref[:half, i, channels:] = total[count + half :]
    ocean_copy.wait()
    last = field_ref[:, width - 1, :]
    first = field_ref[:, 0, :]
    land = ocean_ref[...].astype(F32)
    last_wet = jnp.broadcast_to(land[:, width - 1 : width], (rows, channels))
    first_wet = jnp.broadcast_to(land[:, :1], (rows, channels))
    near_is_last = core == 0
    give_ref[half, :, :channels] = jnp.where(near_is_last, last, first)
    give_ref[half, :, channels:] = jnp.where(near_is_last, last_wet, first_wet)
    away_ref[0, :, :channels] = jnp.where(near_is_last, first, last)
    away_ref[0, :, channels:] = jnp.where(near_is_last, first_wet, last_wet)


def prepare_kernel(
    chips, per, total_lon, modes_ref, local_ref, spectral_ref, ocean_ref, trig_ref, local_out, mix_ref
):
    channels = local_ref.shape[0]
    rows, width = ocean_ref.shape
    wide = 2 * channels
    for t in range(per):
        real, imag = spectral_ref[t, 0], spectral_ref[t, 1]
        top = jnp.concatenate(split(jnp.concatenate([real, imag], 1)), 1)
        low = jnp.concatenate(split(jnp.concatenate([-imag, real], 1)), 1)
        mix_ref[t * wide : t * wide + channels, :] = top
        mix_ref[t * wide + channels : (t + 1) * wide, :] = low
    here = lax.axis_index("lon")
    chip, core = here // 2, lax.rem(here, 2)
    mode_list = []
    for flipped in range(2):
        for d in range(chips):
            source = 2 * gather_source(chip, d, chips) + lax.rem(core + flipped, 2)
            mode_list += [modes_ref[source * per + t] for t in range(per)]
    count = len(mode_list)
    block = width + TAIL
    padded = -(-block // LANES) * LANES
    place = lax.broadcasted_iota(jnp.int32, (count, padded), 1)
    place = jnp.where(place == block - 1, -1, place)
    lon = here * width + place + total_lon
    lon = jnp.where(lon >= total_lon, lon - total_lon, lon)
    lon = jnp.where(lon >= total_lon, lon - total_lon, lon)
    theta = angles(mode_list, lon, total_lon)
    scale = 2.0 / math.sqrt(count)
    table = jnp.concatenate([jnp.cos(theta) * scale, -jnp.sin(theta) * scale], 0)
    high, low = split(table)
    high, low = high.astype(F32), low.astype(F32)
    land = 1.0 - ocean_ref[...].astype(F32)
    land = jnp.concatenate([land, jnp.ones((rows, padded - width), F32)], 1)
    ones = jnp.where(lax.broadcasted_iota(jnp.int32, (8, padded), 0) < 3, 1.0, 0.0)
    stacked = fill([high, low, high, land, ones], trig_ref.shape[1])
    trig_ref[...] = stacked.T[:block].astype(BF16)
    local_out[...] = jnp.concatenate(split(local_ref[...]), 1)


def filter_kernel(conv_ref, out_ref):
    channels = conv_ref.shape[2]
    for col in range(3):
        left = slice(col * channels, (col + 1) * channels)
        right = slice((3 + col) * channels, (4 + col) * channels)
        low, mid, up = (conv_ref[row, col] for row in range(3))
        outer = 0.5 * (low + up)
        for k, taps in enumerate((low, outer + 0.5 * mid, outer - 0.5 * mid, up, mid)):
            top, bottom = split(taps)
            out_ref[k, :channels, left] = top
            out_ref[k, :channels, right] = bottom
            out_ref[k, channels:, left] = top
            out_ref[k, channels:, right] = jnp.zeros_like(top)


def gelu(x):
    inner = math.sqrt(2.0 / math.pi) * (x + 0.044715 * (x * x * x))
    return x * (0.5 * (1.0 + jnp.tanh(inner)))


def mix_kernel(per, rows, *refs):
    summed_ref, *part_refs, mix_ref, out_ref = refs
    wide = summed_ref.shape[1]
    for t in range(per):
        at = slice(t * rows, (t + 1) * rows)
        total = summed_ref[at, :]
        for part in part_refs:
            total = total + part[at, :]
        high, low = split(total)
        weights = mix_ref[t * wide : (t + 1) * wide, :]
        y = dot(high, weights)
        out_ref[at, :] = y[:, :wide] + y[:, wide:] + dot(low, weights[:, :wide])


def hidden_kernel(
    per, field_ref, got_ref, west_ref, east_ref, mixed_ref, trig_ref, local_ref, bias_ref,
    hidden_ref, edge_ref,
):
    rows, width, channels = field_ref.shape
    block = width + TAIL
    count = mixed_ref.shape[0]
    depth = trig_ref.shape[1]
    empty = jnp.zeros((depth, channels), BF16)
    local = local_ref[...]
    south = lax.rem(lax.axis_index("lon"), 2) == 0
    even = lax.rem(lax.axis_index("lat"), 2)
    near = got_ref[got_ref.shape[0] - rows :, :]
    left = jnp.where(south, west_ref[per * rows :, :], near)
    right = jnp.where(south, near, east_ref[per * rows :, :])
    place = lax.broadcasted_iota(jnp.int32, (TAIL, channels), 0)
    first = 6 * count
    lane = lax.broadcasted_iota(jnp.int32, (rows, depth), 1)
    mine = lane == first + lax.broadcasted_iota(jnp.int32, (rows, depth), 0)
    dry = [jnp.sum(jnp.where(mine, 1.0 - side[:, channels : channels + 1], 0.0), 0, keepdims=True) for side in (left, right)]
    tail_place = lax.broadcasted_iota(jnp.int32, (TAIL, depth), 0)
    tail_lane = lax.broadcasted_iota(jnp.int32, (TAIL, depth), 1)
    is_land = (tail_lane >= first) & (tail_lane < first + rows)
    end = trig_ref[width:, :].astype(F32)
    end = jnp.where(is_land & (tail_place == TAIL - 1), dry[0], end)
    end = jnp.where(is_land & (tail_place == 0), dry[1], end)
    trig = jnp.concatenate([trig_ref[:width, :], end.astype(BF16)], 0)
    b_high, b_mid = split(bias_ref[...])
    rest = bias_ref[...] - b_high.astype(F32) - b_mid.astype(F32)
    shape8 = (8, channels)
    row8 = lax.broadcasted_iota(jnp.int32, shape8, 0)
    bias8 = jnp.where(
        row8 == 0, b_high.astype(F32), jnp.where(row8 == 1, b_mid.astype(F32), jnp.where(row8 == 2, rest, 0.0))
    ).astype(F32)
    select = lax.broadcasted_iota(jnp.int32, (rows, channels), 0)
    for i in range(rows):
        side = jnp.where(
            place == TAIL - 1, left[i : i + 1, :channels], jnp.where(place == 0, right[i : i + 1, :channels], 0.0)
        )
        x = jnp.concatenate([field_ref[i], side], 0)
        x_high, x_low = split(x)
        mixed = jnp.concatenate([mixed_ref[:, i, :channels], mixed_ref[:, i, channels:]], 0)
        m_high, m_low = split(mixed)
        cut = jnp.where(select == i, DRY, 0.0)
        extra = jnp.concatenate([cut, bias8], 0).astype(BF16)
        spare = depth - first - extra.shape[0]
        extra = jnp.concatenate([extra, jnp.zeros((spare, channels), BF16)], 0)
        lower = jnp.concatenate([m_high, m_high, m_low, extra], 0)
        rhs = jnp.concatenate([local, jnp.concatenate([lower, empty], 1)], 0)
        lhs = jnp.concatenate([x_high, trig], 1)
        y = dot(lhs, rhs)
        y = gelu(y[:, :channels] + y[:, channels:] + dot(x_low, local[:, :channels]))
        hidden_ref[i * block : (i + 1) * block, :] = y
        if i == 0:
            edge_ref[1 - even] = y
        if i == rows - 1:
            edge_ref[even] = y


def columns(t, channels, keep):
    west = pltpu.roll(t[:, :channels], 1, 0)
    east = pltpu.roll(t[:, 2 * channels :], t.shape[0] - 1, 0)
    return (west + t[:, channels : 2 * channels] + east)[:keep]


def product(parts, weights, channels):
    lhs = jnp.concatenate([jnp.concatenate(split(part), 1) for part in parts], 0)
    y = dot(lhs, weights)
    return y[:, : 3 * channels] + y[:, 3 * channels :]


def inner_kernel(groups, hidden_ref, ocean_ref, bias_ref, filter_ref, out_ref):
    _, width = ocean_ref.shape
    channels = hidden_ref.shape[1]
    block = width + TAIL
    wet = ocean_ref[...].astype(F32).T
    for group in groups:
        terms = [[], [], [], []]
        for first in group:
            d = [hidden_ref[(first - 1 + k) * block : (first + k) * block, :] for k in range(4)]
            terms[0].append(d[0] - d[2])
            terms[1].append(d[1] + d[2])
            terms[2].append(d[2] - d[1])
            terms[3].append(d[1] - d[3])
        m = [product(terms[k], filter_ref[k], channels) for k in range(4)]
        pair = (m[0] + m[1] + m[2], m[1] - m[2] - m[3])
        for g, first in enumerate(group):
            for r in range(2):
                t = columns(pair[r][g * block : (g + 1) * block], channels, width)
                row = first + r
                out_ref[row - 1] = (t + bias_ref[...]) * wet[:, row : row + 1]


def outer_kernel(
    hidden_ref, first_ref, second_ref, ocean_ref, bias_ref, filter_ref, inner_ref, out_ref, buf_ref, sem_ref
):
    rows, width = ocean_ref.shape
    channels = hidden_ref.shape[1]
    block = width + TAIL
    middle = pltpu.make_async_copy(inner_ref, out_ref.at[pl.ds(1, rows - 2)], sem_ref.at[2])
    middle.start()
    wet = ocean_ref[...].astype(F32).T

    def at(row):
        return hidden_ref[row * block : (row + 1) * block, :]

    even = lax.rem(lax.axis_index("lat"), 2) == 0
    above = jnp.where(even, second_ref[0], first_ref[0])
    below = jnp.where(even, first_ref[0], second_ref[0])
    z = product([at(0), at(rows - 1)], filter_ref[4], channels)
    z = z + product([at(1), below], filter_ref[3], channels)
    z = z + product([above, at(rows - 2)], filter_ref[0], channels)
    copies = [middle]
    for r, row in enumerate((0, rows - 1)):
        t = columns(z[r * block : (r + 1) * block], channels, width)
        buf_ref[r] = (t + bias_ref[...]) * wet[:, row : row + 1]
        copy = pltpu.make_async_copy(buf_ref.at[pl.ds(r, 1)], out_ref.at[pl.ds(row, 1)], sem_ref.at[r])
        copy.start()
        copies.append(copy)
    for copy in copies:
        copy.wait()


def vmem():
    return pl.BlockSpec(memory_space=pltpu.VMEM)


def smem():
    return pl.BlockSpec(memory_space=pltpu.SMEM)


def struct(shape, dtype=F32):
    return jax.ShapeDtypeStruct(shape, dtype)


def params(mib):
    return pltpu.CompilerParams(vmem_limit_bytes=mib * MIB)


def per_device(
    field, ocean, modes, spectral_weight, local_weight, layer_bias, conv_weight, conv_bias
):
    rows, width, channels = field.shape
    devices = lax.axis_size("lon")
    chips = devices // 2
    bands = lax.axis_size("lat")
    total_lon = width * devices
    total_modes = modes.shape[0]
    per = total_modes // devices
    half = chips * per
    block = width + TAIL
    steps = distances(chips)
    wide = 2 * channels
    chunks = 2

    give, keep, away = pl.pallas_call(
        functools.partial(forward_kernel, chips, per, total_lon),
        out_shape=(
            struct((half + 1, rows, wide)),
            struct((half, rows, wide)),
            struct((1, rows, wide)),
        ),
        in_specs=[pl.BlockSpec(memory_space=pltpu.MemorySpace.HBM)] * 3,
        out_specs=(vmem(), vmem(), vmem()),
        scratch_shapes=[
            pltpu.SMEM((total_modes,), jnp.int32),
            pltpu.VMEM((rows, width, channels), F32),
            pltpu.VMEM((rows, width), jnp.int32),
            pltpu.SemaphoreType.DMA((2,)),
            pltpu.SemaphoreType.DMA((chunks,)),
        ],
        compiler_params=params(16),
        name="forward",
    )(*[pltpu.with_memory_space_constraint(x, pltpu.MemorySpace.HBM) for x in (modes, field, ocean)])
    give = give.reshape((half + 1) * rows, wide)
    keep = keep.reshape(half * rows, wide)
    away = away.reshape(rows, wide)

    depth = -(-(6 * total_modes + rows + 8) // LANES) * LANES
    trig, local, mix = pl.pallas_call(
        functools.partial(prepare_kernel, chips, per, total_lon),
        out_shape=(
            struct((block, depth), BF16),
            struct((channels, 2 * channels), BF16),
            struct((per * wide, 2 * wide), BF16),
        ),
        in_specs=[smem(), vmem(), vmem(), vmem()],
        out_specs=(vmem(),) * 3,
        compiler_params=params(16),
        name="prepare",
    )(modes, local_weight, spectral_weight, ocean)
    filters = pl.pallas_call(
        filter_kernel,
        out_shape=struct((5, 2 * channels, 6 * channels), BF16),
        in_specs=[vmem()],
        out_specs=vmem(),
        compiler_params=params(16),
        name="filters",
    )(conv_weight)

    got = lax.ppermute(give, "lon", pair_moves(chips))
    summed = keep + got[: half * rows]
    size = per * rows
    parts = {}
    for d in steps:
        send = summed[d * size : (d + 1) * size]
        flip = flip_of(d, chips)
        if flip:
            send = jnp.concatenate([send, away])
        parts[d] = lax.ppermute(send, "lon", chip_moves(d, chips, flip))

    own_mixed = pl.pallas_call(
        functools.partial(mix_kernel, per, rows),
        out_shape=struct((size, wide)),
        in_specs=[vmem()] * (len(steps) + 2),
        out_specs=vmem(),
        compiler_params=params(8),
        name="mix",
    )(summed, *[parts[d] for d in steps], mix)
    gathered = [own_mixed]
    for d in range(1, chips):
        gathered.append(lax.ppermute(own_mixed, "lon", gather_moves(d, chips)))
    gathered = jnp.concatenate(gathered)
    other = lax.ppermute(gathered, "lon", pair_moves(chips))
    mixed = jnp.concatenate([gathered, other]).reshape(total_modes, rows, wide)

    hidden, edge = pl.pallas_call(
        functools.partial(hidden_kernel, per),
        out_shape=(struct((rows * block, channels)), struct((2, block, channels))),
        in_specs=[vmem()] * 8,
        out_specs=(vmem(),) * 2,
        compiler_params=params(24),
        name="hidden",
    )(field, got, parts[1], parts[chips - 1], mixed, trig, local, layer_bias.reshape(1, channels))

    evens = [(i, i + 1) for i in range(0, bands - 1, 2)]
    odds = [(i, i + 1) for i in range(1, bands - 1, 2)]
    first = lax.ppermute(edge[:1], "lat", evens + [(b, a) for a, b in evens])
    second = lax.ppermute(edge[1:], "lat", odds + [(b, a) for a, b in odds])
    bias = conv_bias.reshape(1, channels)
    firsts = list(range(1, rows - 1, 2))
    groups = [firsts[k : k + 2] for k in range(0, len(firsts), 2)]
    if len(groups) > 1 and len(groups[-1]) == 1:
        groups[-2:] = [groups[-2] + groups[-1]]
    flops = 2 * 6 * 4 * rows * width * channels * channels
    inner = pl.pallas_call(
        functools.partial(inner_kernel, groups),
        out_shape=struct((rows - 2, width, channels)),
        in_specs=[vmem()] * 4,
        out_specs=vmem(),
        compiler_params=params(24),
        cost_estimate=pl.CostEstimate(flops=flops, transcendentals=0, bytes_accessed=4 * field.size),
        name="inner",
    )(hidden, ocean, bias, filters)
    return pl.pallas_call(
        outer_kernel,
        out_shape=struct((rows, width, channels)),
        in_specs=[vmem()] * 7,
        out_specs=pl.BlockSpec(memory_space=pl.ANY),
        scratch_shapes=[
            pltpu.VMEM((2, width, channels), F32),
            pltpu.SemaphoreType.DMA((3,)),
        ],
        compiler_params=params(24),
        name="outer",
    )(hidden, first, second, ocean, bias, filters, inner)


def solution(mesh):
    in_specs = (
        P("lat", "lon", None),
        P("lat", "lon"),
        P(),
        P("lon", None, None, None),
        P(),
        P(),
        P(),
        P(),
    )
    out_specs = P("lat", "lon", None)
    return jax.shard_map(
        per_device, mesh=mesh, in_specs=in_specs, out_specs=out_specs, check_vma=False
    )
```

```python
import functools
import math

import jax
import jax.numpy as jnp
from jax import lax
from jax.experimental import pallas as pl
from jax.experimental.pallas import tpu as pltpu
from jax.sharding import PartitionSpec as P

LANES = 128
TAIL = 16
MIB = 1 << 20
DRY = -(2.0**36)
F32 = jnp.float32
BF16 = jnp.bfloat16


def flip_of(distance):
    return 1 if distance & (distance + 1) == 0 and distance else 0


def chip_moves(distance, chips, flip):
    return [
        (2 * chip + core, 2 * (chip ^ distance) + (core ^ flip)) for chip in range(chips) for core in range(2)
    ]


def pair_moves(chips):
    return [(device, device ^ 1) for device in range(2 * chips)]


def split(x):
    high = x.astype(BF16)
    return high, (x - high.astype(F32)).astype(BF16)


def dot(a, b):
    return lax.dot_general(a, b, (((1,), (0,)), ((), ())), preferred_element_type=F32)


def fill(blocks, depth):
    missing = depth - sum(block.shape[0] for block in blocks)
    if missing:
        blocks = blocks + [jnp.zeros((missing,) + blocks[0].shape[1:], blocks[0].dtype)]
    return jnp.concatenate(blocks, 0)


def angles(mode_list, lon, total_lon):
    row = lax.broadcasted_iota(jnp.int32, lon.shape, 0)
    ids = jnp.zeros(lon.shape, jnp.int32)
    for index, mode in enumerate(mode_list):
        ids = jnp.where(row == index, mode, ids)
    product = ids * lon
    if total_lon & (total_lon - 1):
        product = lax.rem(product, total_lon)
    else:
        product = product & (total_lon - 1)
    return product.astype(F32) * (2.0 * math.pi / total_lon)


def forward_kernel(
    chips, per, total_lon, modes_hbm, field_hbm, ocean_hbm, give_ref, keep_ref, away_ref, first_ref, second_ref,
    modes_ref, field_ref, ocean_ref, small_sem, field_sem,
):
    rows, width, channels = field_ref.shape
    chunks = field_sem.shape[0]
    step = rows // chunks
    first_copy = pltpu.make_async_copy(modes_hbm, modes_ref, small_sem.at[0])
    first_copy.start()
    copies = []
    for k in range(chunks):
        part = pl.ds(k * step, step)
        copies.append(pltpu.make_async_copy(field_hbm.at[part], field_ref.at[part], field_sem.at[k]))
        copies[-1].start()
    ocean_copy = pltpu.make_async_copy(ocean_hbm, ocean_ref, small_sem.at[1])
    ocean_copy.start()
    here = lax.axis_index("lon")
    chip, core = here // 2, lax.rem(here, 2)
    first_copy.wait()
    mode_list = []
    for flipped in range(2):
        for d in range(chips):
            owner = 2 * (chip ^ d) + lax.rem(core + flipped + flip_of(d), 2)
            mode_list += [modes_ref[owner * per + t] for t in range(per)]
    count = len(mode_list)
    half = count // 2
    lon = here * width + lax.broadcasted_iota(jnp.int32, (count, width), 1)
    theta = angles(mode_list, lon, total_lon)
    scale = 1.0 / math.sqrt(total_lon)
    table = jnp.concatenate([jnp.cos(theta) * scale, -jnp.sin(theta) * scale], 0)
    lhs = jnp.concatenate(split(table), 0)
    for i in range(rows):
        if i % step == 0:
            copies[i // step].wait()
        rhs = jnp.concatenate(split(field_ref[i]), 1)
        product = dot(lhs, rhs)
        total = product[: 2 * count] + product[2 * count :]
        total = total[:, :channels] + total[:, channels:]
        keep_ref[:half, i, :channels] = total[:half]
        give_ref[:half, i, :channels] = total[half:count]
        keep_ref[:half, i, channels:] = total[count : count + half]
        give_ref[:half, i, channels:] = total[count + half :]
    ocean_copy.wait()
    last = field_ref[:, width - 1, :]
    first = field_ref[:, 0, :]
    land = ocean_ref[...].astype(F32)
    last_wet = jnp.broadcast_to(land[:, width - 1 : width], (rows, channels))
    first_wet = jnp.broadcast_to(land[:, :1], (rows, channels))
    even = lax.rem(lax.axis_index("lat"), 2) == 0
    for out, at_end in ((first_ref, even), (second_ref, ~even)):
        out[:width, :] = jnp.where(at_end, field_ref[rows - 1], field_ref[0])
        row = jnp.where(at_end, land[rows - 1 :], land[:1])
        pieces = [row[:, k : k + channels] for k in range(0, width, channels)]
        out[width:, :] = fill(pieces, out.shape[0] - width)
    near_is_last = core == 0
    give_ref[half, :, :channels] = jnp.where(near_is_last, last, first)
    give_ref[half, :, channels:] = jnp.where(near_is_last, last_wet, first_wet)
    away_ref[0, :, :channels] = jnp.where(near_is_last, first, last)
    away_ref[0, :, channels:] = jnp.where(near_is_last, first_wet, last_wet)


def prepare_kernel(
    chips, per, total_lon, modes_ref, local_ref, spectral_ref, ocean_ref, trig_ref, local_out, mix_ref
):
    channels = local_ref.shape[0]
    rows, width = ocean_ref.shape
    wide = 2 * channels
    for t in range(per):
        real, imag = spectral_ref[t, 0], spectral_ref[t, 1]
        top = jnp.concatenate(split(jnp.concatenate([real, imag], 1)), 1)
        low = jnp.concatenate(split(jnp.concatenate([-imag, real], 1)), 1)
        mix_ref[t * wide : t * wide + channels, :] = top
        mix_ref[t * wide + channels : (t + 1) * wide, :] = low
    here = lax.axis_index("lon")
    chip, core = here // 2, lax.rem(here, 2)
    mode_list = []
    for flipped in range(2):
        for d in range(chips):
            source = 2 * (chip ^ d) + lax.rem(core + flipped, 2)
            mode_list += [modes_ref[source * per + t] for t in range(per)]
    count = len(mode_list)
    block = width + TAIL
    padded = -(-block // LANES) * LANES
    place = lax.broadcasted_iota(jnp.int32, (count, padded), 1)
    place = jnp.where(place == block - 1, -1, place)
    lon = here * width + place + total_lon
    lon = jnp.where(lon >= total_lon, lon - total_lon, lon)
    lon = jnp.where(lon >= total_lon, lon - total_lon, lon)
    theta = angles(mode_list, lon, total_lon)
    scale = 2.0 / math.sqrt(count)
    table = jnp.concatenate([jnp.cos(theta) * scale, -jnp.sin(theta) * scale], 0)
    high, low = split(table)
    high, low = high.astype(F32), low.astype(F32)
    land = 1.0 - ocean_ref[...].astype(F32)
    land = jnp.concatenate([land, jnp.ones((rows, padded - width), F32)], 1)
    ones = jnp.where(lax.broadcasted_iota(jnp.int32, (8, padded), 0) < 3, 1.0, 0.0)
    stacked = fill([high, low, high, land, ones], trig_ref.shape[1])
    trig_ref[...] = stacked.T[:block].astype(BF16)
    local_out[...] = jnp.concatenate(split(local_ref[...]), 1)


def filter_kernel(conv_ref, out_ref):
    channels = conv_ref.shape[2]
    for col in range(3):
        left = slice(col * channels, (col + 1) * channels)
        right = slice((3 + col) * channels, (4 + col) * channels)
        low, mid, up = (0.5 * conv_ref[row, col] for row in range(3))
        outer = 0.5 * (low + up)
        for k, taps in enumerate((low, outer + 0.5 * mid, outer - 0.5 * mid, up, mid)):
            top, bottom = split(taps)
            out_ref[k, :channels, left] = top
            out_ref[k, :channels, right] = bottom
            out_ref[k, channels:, left] = top
            out_ref[k, channels:, right] = jnp.zeros_like(top)


def twice_gelu(x):
    slope = math.sqrt(2.0 / math.pi)
    return x * (1.0 + jnp.tanh(x * (slope + (slope * 0.044715) * (x * x))))


def hidden_rows(x, mixed, cut, trig, local, bias, channels):
    depth = trig.shape[1]
    x_high, x_low = split(x)
    m_high, m_low = split(mixed)
    lower = fill([m_high, m_high, m_low, jnp.concatenate([cut, bias], 0).astype(BF16)], depth)
    rhs = jnp.concatenate([lower, jnp.zeros((depth, channels), BF16)], 1)
    rhs = jnp.concatenate([local, rhs], 0)
    y = dot(jnp.concatenate([x_high, trig], 1), rhs)
    return twice_gelu(y[:, :channels] + y[:, channels:] + dot(x_low, local[:, :channels]))


def bias_rows(bias_ref):
    high, mid = split(bias_ref[...])
    high, mid = high.astype(F32), mid.astype(F32)
    row = lax.broadcasted_iota(jnp.int32, (8, high.shape[1]), 0)
    rest = jnp.where(row == 2, bias_ref[...] - high - mid, 0.0)
    return jnp.where(row == 0, high, jnp.where(row == 1, mid, rest))


def side_columns(chips, per, rows, got_ref, far_refs):
    here = lax.axis_index("lon")
    chip, south = here // 2, lax.rem(here, 2) == 0
    other = lax.rem(jnp.where(south, chip + chips - 1, chip + 1), chips)
    far = far_refs[0][per * rows :, :]
    masks = [d for d in range(chips) if flip_of(d)]
    for d, ref in zip(masks[1:], far_refs[1:]):
        far = jnp.where((chip ^ other) == d, ref[per * rows :, :], far)
    near = got_ref[got_ref.shape[0] - rows :, :]
    return jnp.where(south, far, near), jnp.where(south, near, far)


def edges_kernel(chips, per, got_ref, mixed_ref, *refs):
    *far_refs, first_ref, second_ref = refs
    count, rows, _ = mixed_ref.shape
    left, right = side_columns(chips, per, rows, got_ref, far_refs)
    even = lax.rem(lax.axis_index("lat"), 2) == 0
    for out, at_end in ((first_ref, even), (second_ref, ~even)):
        out[:count, :] = jnp.where(at_end, mixed_ref[:, rows - 1, :], mixed_ref[:, 0, :])
        sides = [jnp.where(at_end, side[rows - 1 :], side[:1]) for side in (left, right)]
        out[count:, :] = fill(sides, out.shape[0] - count)


def mix_kernel(per, rows, *refs):
    summed_ref, *part_refs, mix_ref, out_ref = refs
    wide = summed_ref.shape[1]
    for t in range(per):
        at = slice(t * rows, (t + 1) * rows)
        total = summed_ref[at, :]
        for part in part_refs:
            total = total + part[at, :]
        high, low = split(total)
        weights = mix_ref[t * wide : (t + 1) * wide, :]
        y = dot(high, weights)
        out_ref[at, :] = y[:, :wide] + y[:, wide:] + dot(low, weights[:, :wide])


def hidden_kernel(chips, per, field_ref, got_ref, mixed_ref, trig_ref, local_ref, bias_ref, *refs):
    *far_refs, hidden_ref = refs
    rows, width, channels = field_ref.shape
    block = width + TAIL
    count = mixed_ref.shape[0]
    depth = trig_ref.shape[1]
    local = local_ref[...]
    left, right = side_columns(chips, per, rows, got_ref, far_refs)
    place = lax.broadcasted_iota(jnp.int32, (TAIL, channels), 0)
    first = 6 * count
    lane = lax.broadcasted_iota(jnp.int32, (rows, depth), 1)
    mine = lane == first + lax.broadcasted_iota(jnp.int32, (rows, depth), 0)
    dry = [
        jnp.sum(jnp.where(mine, 1.0 - side[:, channels : channels + 1], 0.0), 0, keepdims=True)
        for side in (left, right)
    ]
    tail_place = lax.broadcasted_iota(jnp.int32, (TAIL, depth), 0)
    tail_lane = lax.broadcasted_iota(jnp.int32, (TAIL, depth), 1)
    is_land = (tail_lane >= first) & (tail_lane < first + rows)
    end = trig_ref[width:, :].astype(F32)
    end = jnp.where(is_land & (tail_place == TAIL - 1), dry[0], end)
    end = jnp.where(is_land & (tail_place == 0), dry[1], end)
    trig = jnp.concatenate([trig_ref[:width, :], end.astype(BF16)], 0)
    bias = bias_rows(bias_ref)
    select = lax.broadcasted_iota(jnp.int32, (rows, channels), 0)
    for i in range(rows):
        side = jnp.where(
            place == TAIL - 1, left[i : i + 1, :channels], jnp.where(place == 0, right[i : i + 1, :channels], 0.0)
        )
        x = jnp.concatenate([field_ref[i], side], 0)
        mixed = jnp.concatenate([mixed_ref[:, i, :channels], mixed_ref[:, i, channels:]], 0)
        cut = jnp.where(select == i, DRY, 0.0)
        hidden_ref[i * block : (i + 1) * block, :] = hidden_rows(x, mixed, cut, trig, local, bias, channels)


def columns(t, channels, keep):
    west = pltpu.roll(t[:, :channels], 1, 0)
    east = pltpu.roll(t[:, 2 * channels :], t.shape[0] - 1, 0)
    return (west + t[:, channels : 2 * channels] + east)[:keep]


def product(parts, weights, channels):
    lhs = jnp.concatenate([jnp.concatenate(split(part), 1) for part in parts], 0)
    y = dot(lhs, weights)
    return y[:, : 3 * channels] + y[:, 3 * channels :]


def inner_kernel(groups, hidden_ref, ocean_ref, bias_ref, filter_ref, out_ref):
    _, width = ocean_ref.shape
    channels = hidden_ref.shape[1]
    block = width + TAIL
    wet = ocean_ref[...].astype(F32).T
    for group in groups:
        terms = [[], [], [], []]
        for first in group:
            d = [hidden_ref[(first - 1 + k) * block : (first + k) * block, :] for k in range(4)]
            terms[0].append(d[0] - d[2])
            terms[1].append(d[1] + d[2])
            terms[2].append(d[2] - d[1])
            terms[3].append(d[1] - d[3])
        m = [product(terms[k], filter_ref[k], channels) for k in range(4)]
        pair = (m[0] + m[1] + m[2], m[1] - m[2] - m[3])
        for g, first in enumerate(group):
            for r in range(2):
                t = columns(pair[r][g * block : (g + 1) * block], channels, width)
                row = first + r
                out_ref[row - 1] = (t + bias_ref[...]) * wet[:, row : row + 1]


def outer_kernel(
    bands, hidden_ref, early_first, early_second, late_first, late_second, trig_ref, local_ref, layer_ref,
    ocean_ref, bias_ref, filter_ref, inner_ref, out_ref, buf_ref, sem_ref,
):
    rows, width = ocean_ref.shape
    channels = hidden_ref.shape[1]
    block = width + TAIL
    middle = pltpu.make_async_copy(inner_ref, out_ref.at[pl.ds(1, rows - 2)], sem_ref.at[2])
    middle.start()
    wet = ocean_ref[...].astype(F32).T
    layer = bias_rows(layer_ref)
    no_cut = jnp.zeros((rows, channels), F32)
    place = lax.broadcasted_iota(jnp.int32, (TAIL, channels), 0)

    def neighbour(early, late):
        count = late.shape[0] - 8
        left, right = late[count : count + 1, :], late[count + 1 : count + 2, :]

        def tail(lanes):
            return jnp.where(place == TAIL - 1, left[:, lanes], jnp.where(place == 0, right[:, lanes], 0.0))

        flags = early[width:, :].T
        pieces = [jnp.broadcast_to(flags[:, k : k + 1], (channels, channels)) for k in range(width // channels)]
        mask = jnp.concatenate(pieces + [tail(slice(channels, None))], 0)
        x = jnp.concatenate([early[:width, :], tail(slice(0, channels))], 0)
        mixed = jnp.concatenate([late[:count, :channels], late[:count, channels:]], 0)
        return mask * hidden_rows(x, mixed, no_cut, trig_ref[...], local_ref[...], layer, channels)

    def at(row):
        return hidden_ref[row * block : (row + 1) * block, :]

    band = lax.axis_index("lat")
    even = lax.rem(band, 2) == 0
    one = neighbour(early_first, late_first)
    two = neighbour(early_second, late_second)
    above = jnp.where(band == 0, 0.0, jnp.where(even, two, one))
    below = jnp.where(band == bands - 1, 0.0, jnp.where(even, one, two))
    z = product([at(0), at(rows - 1)], filter_ref[4], channels)
    z = z + product([at(1), below], filter_ref[3], channels)
    z = z + product([above, at(rows - 2)], filter_ref[0], channels)
    copies = [middle]
    for r, row in enumerate((0, rows - 1)):
        t = columns(z[r * block : (r + 1) * block], channels, width)
        buf_ref[r] = (t + bias_ref[...]) * wet[:, row : row + 1]
        copy = pltpu.make_async_copy(buf_ref.at[pl.ds(r, 1)], out_ref.at[pl.ds(row, 1)], sem_ref.at[r])
        copy.start()
        copies.append(copy)
    for copy in copies:
        copy.wait()


def vmem():
    return pl.BlockSpec(memory_space=pltpu.VMEM)


def smem():
    return pl.BlockSpec(memory_space=pltpu.SMEM)


def struct(shape, dtype=F32):
    return jax.ShapeDtypeStruct(shape, dtype)


def params(mib):
    return pltpu.CompilerParams(vmem_limit_bytes=mib * MIB)


def per_device(
    field, ocean, modes, spectral_weight, local_weight, layer_bias, conv_weight, conv_bias
):
    rows, width, channels = field.shape
    devices = lax.axis_size("lon")
    chips = devices // 2
    bands = lax.axis_size("lat")
    total_lon = width * devices
    total_modes = modes.shape[0]
    per = total_modes // devices
    half = chips * per
    block = width + TAIL
    steps = list(range(1, chips))
    wide = 2 * channels
    chunks = 2

    give, keep, away, early_first, early_second = pl.pallas_call(
        functools.partial(forward_kernel, chips, per, total_lon),
        out_shape=(
            struct((half + 1, rows, wide)),
            struct((half, rows, wide)),
            struct((1, rows, wide)),
            struct((width + 8, channels)),
            struct((width + 8, channels)),
        ),
        in_specs=[pl.BlockSpec(memory_space=pltpu.MemorySpace.HBM)] * 3,
        out_specs=(vmem(),) * 5,
        scratch_shapes=[
            pltpu.SMEM((total_modes,), jnp.int32),
            pltpu.VMEM((rows, width, channels), F32),
            pltpu.VMEM((rows, width), jnp.int32),
            pltpu.SemaphoreType.DMA((2,)),
            pltpu.SemaphoreType.DMA((chunks,)),
        ],
        compiler_params=params(16),
        name="forward",
    )(*[pltpu.with_memory_space_constraint(x, pltpu.MemorySpace.HBM) for x in (modes, field, ocean)])
    give = give.reshape((half + 1) * rows, wide)
    keep = keep.reshape(half * rows, wide)
    away = away.reshape(rows, wide)

    depth = -(-(6 * total_modes + rows + 8) // LANES) * LANES
    trig, local, mix = pl.pallas_call(
        functools.partial(prepare_kernel, chips, per, total_lon),
        out_shape=(
            struct((block, depth), BF16),
            struct((channels, 2 * channels), BF16),
            struct((per * wide, 2 * wide), BF16),
        ),
        in_specs=[smem(), vmem(), vmem(), vmem()],
        out_specs=(vmem(),) * 3,
        compiler_params=params(16),
        name="prepare",
    )(modes, local_weight, spectral_weight, ocean)
    filters = pl.pallas_call(
        filter_kernel,
        out_shape=struct((5, 2 * channels, 6 * channels), BF16),
        in_specs=[vmem()],
        out_specs=vmem(),
        compiler_params=params(16),
        name="filters",
    )(conv_weight)

    got = lax.ppermute(give, "lon", pair_moves(chips))
    summed = keep + got[: half * rows]
    size = per * rows
    parts = {}
    for d in steps:
        send = summed[d * size : (d + 1) * size]
        if flip_of(d):
            send = jnp.concatenate([send, away])
        parts[d] = lax.ppermute(send, "lon", chip_moves(d, chips, flip_of(d)))
    crossed = [parts[d] for d in steps if flip_of(d)]
    evens = [(i, i + 1) for i in range(0, bands - 1, 2)]
    odds = [(i, i + 1) for i in range(1, bands - 1, 2)]
    if bands % 2 == 0 and bands > 2:
        odds.append((0, bands - 1))
    evens, odds = ([(a, b) for a, b in moves] + [(b, a) for a, b in moves] for moves in (evens, odds))
    early_first = lax.ppermute(early_first, "lat", evens)
    early_second = lax.ppermute(early_second, "lat", odds)

    own_mixed = pl.pallas_call(
        functools.partial(mix_kernel, per, rows),
        out_shape=struct((size, wide)),
        in_specs=[vmem()] * (len(steps) + 2),
        out_specs=vmem(),
        compiler_params=params(8),
        name="mix",
    )(summed, *[parts[d] for d in steps], mix)
    gathered = [own_mixed]
    for d in steps:
        gathered.append(lax.ppermute(own_mixed, "lon", chip_moves(d, chips, 0)))
    gathered = jnp.concatenate(gathered)
    other = lax.ppermute(gathered, "lon", pair_moves(chips))
    mixed = jnp.concatenate([gathered, other]).reshape(total_modes, rows, wide)

    late = struct((total_modes + 8, wide))
    late_first, late_second = pl.pallas_call(
        functools.partial(edges_kernel, chips, per),
        out_shape=(late, late),
        in_specs=[vmem()] * (2 + len(crossed)),
        out_specs=(vmem(),) * 2,
        compiler_params=params(8),
        name="edges",
    )(got, mixed, *crossed)
    late_first = lax.ppermute(late_first, "lat", evens)
    late_second = lax.ppermute(late_second, "lat", odds)
    layer = layer_bias.reshape(1, channels)
    hidden = pl.pallas_call(
        functools.partial(hidden_kernel, chips, per),
        out_shape=struct((rows * block, channels)),
        in_specs=[vmem()] * (6 + len(crossed)),
        out_specs=vmem(),
        compiler_params=params(24),
        cost_estimate=pl.CostEstimate(
            flops=6 * 256 * rows * width * channels, transcendentals=field.size, bytes_accessed=4 * field.size
        ),
        name="hidden",
    )(field, got, mixed, trig, local, layer, *crossed)

    bias = conv_bias.reshape(1, channels)
    firsts = list(range(1, rows - 1, 2))
    groups = [firsts[k : k + 2] for k in range(0, len(firsts), 2)]
    if len(groups) > 1 and len(groups[-1]) == 1:
        groups[-2:] = [groups[-2] + groups[-1]]
    flops = 2 * 6 * 4 * rows * width * channels * channels
    inner = pl.pallas_call(
        functools.partial(inner_kernel, groups),
        out_shape=struct((rows - 2, width, channels)),
        in_specs=[vmem()] * 4,
        out_specs=vmem(),
        compiler_params=params(24),
        cost_estimate=pl.CostEstimate(flops=flops, transcendentals=0, bytes_accessed=4 * field.size),
        name="inner",
    )(hidden, ocean, bias, filters)
    return pl.pallas_call(
        functools.partial(outer_kernel, bands),
        out_shape=struct((rows, width, channels)),
        in_specs=[vmem()] * 12,
        out_specs=pl.BlockSpec(memory_space=pl.ANY),
        scratch_shapes=[
            pltpu.VMEM((2, width, channels), F32),
            pltpu.SemaphoreType.DMA((3,)),
        ],
        compiler_params=params(24),
        name="outer",
    )(
        hidden, early_first, early_second, late_first, late_second, trig, local, layer, ocean, bias, filters, inner
    )


def solution(mesh):
    in_specs = (
        P("lat", "lon", None),
        P("lat", "lon"),
        P(),
        P("lon", None, None, None),
        P(),
        P(),
        P(),
        P(),
    )
    out_specs = P("lat", "lon", None)
    return jax.shard_map(
        per_device, mesh=mesh, in_specs=in_specs, out_specs=out_specs, check_vma=False
    )
```

```python
import functools
import math

import jax
import jax.numpy as jnp
from jax import lax
from jax.experimental import pallas as pl
from jax.experimental.pallas import tpu as pltpu
from jax.sharding import PartitionSpec as P

LANES = 128
TAIL = 8
MIB = 1 << 20
DRY = -(2.0**36)
F32 = jnp.float32
BF16 = jnp.bfloat16


def flip_of(distance):
    return 1 if distance & (distance + 1) == 0 and distance else 0


def chip_moves(distance, chips, flip):
    return [
        (2 * chip + core, 2 * (chip ^ distance) + (core ^ flip)) for chip in range(chips) for core in range(2)
    ]


def pair_moves(chips):
    return [(device, device ^ 1) for device in range(2 * chips)]


def split(x):
    high = x.astype(BF16)
    return high, (x - high.astype(F32)).astype(BF16)


def dot(a, b):
    return lax.dot_general(a, b, (((1,), (0,)), ((), ())), preferred_element_type=F32)


def fill(blocks, depth):
    missing = depth - sum(block.shape[0] for block in blocks)
    if missing:
        blocks = blocks + [jnp.zeros((missing,) + blocks[0].shape[1:], blocks[0].dtype)]
    return jnp.concatenate(blocks, 0)


def angles(mode_list, lon, total_lon):
    row = lax.broadcasted_iota(jnp.int32, lon.shape, 0)
    ids = jnp.zeros(lon.shape, jnp.int32)
    for index, mode in enumerate(mode_list):
        ids = jnp.where(row == index, mode, ids)
    return turns(ids * lon, total_lon)


def turns(product, total_lon):
    if total_lon & (total_lon - 1):
        product = lax.rem(product, total_lon)
    else:
        product = product & (total_lon - 1)
    return product.astype(F32) * (2.0 * math.pi / total_lon)


def forward_kernel(
    chips, per, total_lon, modes_hbm, field_hbm, ocean_hbm, give_ref, keep_ref, away_ref, first_ref, second_ref,
    high_ref, low_ref,     modes_ref, field_ref, ocean_ref, small_sem, field_sem,
):
    rows, width, channels = field_ref.shape
    chunks = field_sem.shape[0]
    step = rows // chunks
    first_copy = pltpu.make_async_copy(modes_hbm, modes_ref, small_sem.at[0])
    first_copy.start()
    copies = []
    for k in range(chunks):
        part = pl.ds(k * step, step)
        copies.append(pltpu.make_async_copy(field_hbm.at[part], field_ref.at[part], field_sem.at[k]))
        copies[-1].start()
    ocean_copy = pltpu.make_async_copy(ocean_hbm, ocean_ref, small_sem.at[1])
    ocean_copy.start()
    here = lax.axis_index("lon")
    chip, core = here // 2, lax.rem(here, 2)
    first_copy.wait()
    mode_list = []
    for flipped in range(2):
        for d in range(chips):
            owner = 2 * (chip ^ d) + lax.rem(core + flipped + flip_of(d), 2)
            mode_list += [modes_ref[owner * per + t] for t in range(per)]
    count = len(mode_list)
    half = count // 2
    lon = here * width + lax.broadcasted_iota(jnp.int32, (count, width), 1)
    theta = angles(mode_list, lon, total_lon)
    scale = 1.0 / math.sqrt(total_lon)
    table = jnp.concatenate([jnp.cos(theta) * scale, -jnp.sin(theta) * scale], 0)
    lhs = jnp.concatenate(split(table), 0)
    for i in range(rows):
        if i % step == 0:
            copies[i // step].wait()
        high, low = split(field_ref[i])
        high_ref[i] = high
        low_ref[i] = low
        product = dot(lhs, jnp.concatenate([high, low], 1))
        total = product[: 2 * count] + product[2 * count :]
        total = total[:, :channels] + total[:, channels:]
        keep_ref[:half, i, :channels] = total[:half]
        give_ref[:half, i, :channels] = total[half:count]
        keep_ref[:half, i, channels:] = total[count : count + half]
        give_ref[:half, i, channels:] = total[count + half :]
    ocean_copy.wait()
    last = field_ref[:, width - 1, :]
    first = field_ref[:, 0, :]
    land = ocean_ref[...].astype(F32)
    last_wet = jnp.broadcast_to(land[:, width - 1 : width], (rows, channels))
    first_wet = jnp.broadcast_to(land[:, :1], (rows, channels))
    even = lax.rem(lax.axis_index("lat"), 2) == 0
    for out, at_end in ((first_ref, even), (second_ref, ~even)):
        out[:width, :] = jnp.where(at_end, field_ref[rows - 1], field_ref[0])
        row = jnp.where(at_end, land[rows - 1 :], land[:1])
        pieces = [row[:, k : k + channels] for k in range(0, width, channels)]
        out[width:, :] = fill(pieces, out.shape[0] - width)
    near_is_last = core == 0
    give_ref[half, :, :channels] = jnp.where(near_is_last, last, first)
    give_ref[half, :, channels:] = jnp.where(near_is_last, last_wet, first_wet)
    away_ref[0, :, :channels] = jnp.where(near_is_last, first, last)
    away_ref[0, :, channels:] = jnp.where(near_is_last, first_wet, last_wet)


def prepare_kernel(
    chips, per, total_lon, modes_ref, local_ref, spectral_ref, ocean_ref, trig_ref, local_out, mix_ref
):
    channels = local_ref.shape[0]
    rows, width = ocean_ref.shape
    wide = 2 * channels
    for t in range(per):
        real, imag = spectral_ref[t, 0], spectral_ref[t, 1]
        top = jnp.concatenate(split(jnp.concatenate([real, imag], 1)), 1)
        low = jnp.concatenate(split(jnp.concatenate([-imag, real], 1)), 1)
        mix_ref[t * wide : t * wide + channels, :] = top
        mix_ref[t * wide + channels : (t + 1) * wide, :] = low
    here = lax.axis_index("lon")
    chip, core = here // 2, lax.rem(here, 2)
    count = modes_ref.shape[1]
    spot = lax.broadcasted_iota(jnp.int32, (count, count), 0)
    slot = lax.div(spot, per)
    flipped, d = lax.div(slot, chips), lax.rem(slot, chips)
    source = 2 * (chip ^ d) + (core ^ flipped)
    wanted = source * per + lax.rem(spot, per)
    hit = wanted == lax.broadcasted_iota(jnp.int32, (count, count), 1)
    mine = jnp.sum(jnp.where(hit, modes_ref[...].astype(F32), 0.0), 1, keepdims=True).astype(jnp.int32)
    block = width + TAIL
    padded = -(-block // LANES) * LANES
    place = lax.broadcasted_iota(jnp.int32, (count, padded), 1)
    place = jnp.where(place == block - 1, -1, place)
    lon = here * width + place + total_lon
    lon = jnp.where(lon >= total_lon, lon - total_lon, lon)
    lon = jnp.where(lon >= total_lon, lon - total_lon, lon)
    theta = turns(mine * lon, total_lon)
    scale = 2.0 / math.sqrt(count)
    table = jnp.concatenate([jnp.cos(theta) * scale, -jnp.sin(theta) * scale], 0)
    high, low = split(table)
    high, low = high.astype(F32), low.astype(F32)
    land = 1.0 - ocean_ref[...].astype(F32)
    land = jnp.concatenate([land, jnp.ones((rows, padded - width), F32)], 1)
    ones = jnp.where(lax.broadcasted_iota(jnp.int32, (8, padded), 0) < 3, 1.0, 0.0)
    stacked = fill([high, low, high, land, ones], trig_ref.shape[1])
    trig_ref[...] = stacked.T[:block].astype(BF16)
    local_out[...] = jnp.concatenate(split(local_ref[...]), 1)


def filter_kernel(conv_ref, out_ref):
    channels = conv_ref.shape[2]
    for col in range(3):
        left = slice(col * channels, (col + 1) * channels)
        right = slice((3 + col) * channels, (4 + col) * channels)
        low, mid, up = (0.5 * conv_ref[row, col] for row in range(3))
        outer = 0.5 * (low + up)
        for k, taps in enumerate((low, outer + 0.5 * mid, outer - 0.5 * mid, up, mid)):
            top, bottom = split(taps)
            out_ref[k, :channels, left] = top
            out_ref[k, :channels, right] = bottom
            out_ref[k, channels:, left] = top
            out_ref[k, channels:, right] = jnp.zeros_like(top)


def twice_gelu(x):
    slope = math.sqrt(2.0 / math.pi)
    return x * (1.0 + jnp.tanh(x * (slope + (slope * 0.044715) * (x * x))))


def hidden_pair(parts, mixed, cuts, trig, local, bias, channels):
    depth = trig.shape[1]
    top = local[:, :channels]
    none = jnp.zeros_like(top)
    both = jnp.concatenate([jnp.concatenate([top, none], 1), jnp.concatenate([none, top], 1)], 0)
    rest = dot(jnp.concatenate([parts[0][1], parts[1][1]], 1), both)
    out = []
    for r in range(2):
        m_high, m_low = split(mixed[r])
        lower = fill([m_high, m_high, m_low, jnp.concatenate([cuts[r], bias], 0).astype(BF16)], depth)
        rhs = jnp.concatenate([lower, jnp.zeros((depth, channels), BF16)], 1)
        y = dot(jnp.concatenate([parts[r][0], trig], 1), jnp.concatenate([local, rhs], 0))
        out.append(twice_gelu(y[:, :channels] + y[:, channels:] + rest[:, r * channels : (r + 1) * channels]))
    return out


def bias_rows(bias_ref):
    high, mid = split(bias_ref[...])
    high, mid = high.astype(F32), mid.astype(F32)
    row = lax.broadcasted_iota(jnp.int32, (8, high.shape[1]), 0)
    rest = jnp.where(row == 2, bias_ref[...] - high - mid, 0.0)
    return jnp.where(row == 0, high, jnp.where(row == 1, mid, rest))


def side_columns(chips, per, rows, got_ref, far_refs):
    here = lax.axis_index("lon")
    chip, south = here // 2, lax.rem(here, 2) == 0
    other = lax.rem(jnp.where(south, chip + chips - 1, chip + 1), chips)
    far = far_refs[0][per * rows :, :]
    masks = [d for d in range(chips) if flip_of(d)]
    for d, ref in zip(masks[1:], far_refs[1:]):
        far = jnp.where((chip ^ other) == d, ref[per * rows :, :], far)
    near = got_ref[got_ref.shape[0] - rows :, :]
    return jnp.where(south, far, near), jnp.where(south, near, far)


def edges_kernel(chips, per, got_ref, mixed_ref, *refs):
    *far_refs, first_ref, second_ref = refs
    count, rows, _ = mixed_ref.shape
    left, right = side_columns(chips, per, rows, got_ref, far_refs)
    even = lax.rem(lax.axis_index("lat"), 2) == 0
    for out, at_end in ((first_ref, even), (second_ref, ~even)):
        out[:count, :] = jnp.where(at_end, mixed_ref[:, rows - 1, :], mixed_ref[:, 0, :])
        sides = [jnp.where(at_end, side[rows - 1 :], side[:1]) for side in (left, right)]
        out[count:, :] = fill(sides, out.shape[0] - count)


def mix_kernel(per, rows, *refs):
    summed_ref, *part_refs, mix_ref, out_ref = refs
    wide = summed_ref.shape[1]
    for t in range(per):
        at = slice(t * rows, (t + 1) * rows)
        total = summed_ref[at, :]
        for part in part_refs:
            total = total + part[at, :]
        high, low = split(total)
        weights = mix_ref[t * wide : (t + 1) * wide, :]
        y = dot(high, weights)
        out_ref[at, :] = y[:, :wide] + y[:, wide:] + dot(low, weights[:, :wide])


def hidden_kernel(chips, per, high_ref, low_ref, got_ref, mixed_ref, trig_ref, local_ref, bias_ref, *refs):
    *far_refs, hidden_ref = refs
    rows, width, channels = high_ref.shape
    block = width + TAIL
    count = mixed_ref.shape[0]
    depth = trig_ref.shape[1]
    local = local_ref[...]
    left, right = side_columns(chips, per, rows, got_ref, far_refs)
    place = lax.broadcasted_iota(jnp.int32, (TAIL, channels), 0)
    first = 6 * count
    lane = lax.broadcasted_iota(jnp.int32, (rows, depth), 1)
    mine = lane == first + lax.broadcasted_iota(jnp.int32, (rows, depth), 0)
    dry = [
        jnp.sum(jnp.where(mine, 1.0 - side[:, channels : channels + 1], 0.0), 0, keepdims=True)
        for side in (left, right)
    ]
    tail_place = lax.broadcasted_iota(jnp.int32, (TAIL, depth), 0)
    tail_lane = lax.broadcasted_iota(jnp.int32, (TAIL, depth), 1)
    is_land = (tail_lane >= first) & (tail_lane < first + rows)
    end = trig_ref[width:, :].astype(F32)
    end = jnp.where(is_land & (tail_place == TAIL - 1), dry[0], end)
    end = jnp.where(is_land & (tail_place == 0), dry[1], end)
    trig = jnp.concatenate([trig_ref[:width, :], end.astype(BF16)], 0)
    bias = bias_rows(bias_ref)
    select = lax.broadcasted_iota(jnp.int32, (rows, channels), 0)
    for i in range(0, rows, 2):
        parts, mixed, cuts = [], [], []
        for r in (i, i + 1):
            side = jnp.where(
                place == TAIL - 1, left[r : r + 1, :channels], jnp.where(place == 0, right[r : r + 1, :channels], 0.0)
            )
            high, low = split(side)
            parts.append((jnp.concatenate([high_ref[r], high], 0), jnp.concatenate([low_ref[r], low], 0)))
            mixed.append(jnp.concatenate([mixed_ref[:, r, :channels], mixed_ref[:, r, channels:]], 0))
            cuts.append(jnp.where(select == r, DRY, 0.0))
        pair = hidden_pair(parts, mixed, cuts, trig, local, bias, channels)
        for r in range(2):
            hidden_ref[(i + r) * block : (i + r + 1) * block, :] = pair[r]


def columns(t, channels, keep):
    west = pltpu.roll(t[:, :channels], 1, 0)
    east = pltpu.roll(t[:, 2 * channels :], t.shape[0] - 1, 0)
    return (west + t[:, channels : 2 * channels] + east)[:keep]


def product(parts, weights, channels):
    y = dot(jnp.concatenate(split(jnp.concatenate(parts, 0)), 1), weights)
    return y[:, : 3 * channels] + y[:, 3 * channels :]


def inner_kernel(groups, hidden_ref, ocean_ref, bias_ref, filter_ref, out_ref):
    _, width = ocean_ref.shape
    channels = hidden_ref.shape[1]
    block = width + TAIL
    wet = ocean_ref[...].astype(F32).T
    for group in groups:
        terms = [[], [], [], []]
        for first in group:
            d = [hidden_ref[(first - 1 + k) * block : (first + k) * block, :] for k in range(4)]
            terms[0].append(d[0] - d[2])
            terms[1].append(d[1] + d[2])
            terms[2].append(d[2] - d[1])
            terms[3].append(d[1] - d[3])
        m = [product(terms[k], filter_ref[k], channels) for k in range(4)]
        pair = (m[0] + m[1] + m[2], m[1] - m[2] - m[3])
        for g, first in enumerate(group):
            for r in range(2):
                t = columns(pair[r][g * block : (g + 1) * block], channels, width)
                row = first + r
                out_ref[row - 1] = (t + bias_ref[...]) * wet[:, row : row + 1]


def outer_kernel(
    bands, hidden_ref, early_first, early_second, late_first, late_second, trig_ref, local_ref, layer_ref,
    ocean_ref, bias_ref, filter_ref, inner_ref, out_ref, buf_ref, sem_ref,
):
    rows, width = ocean_ref.shape
    channels = local_ref.shape[0]
    block = width + TAIL
    middle = pltpu.make_async_copy(inner_ref, out_ref.at[pl.ds(1, rows - 2)], sem_ref.at[2])
    middle.start()
    wet = ocean_ref[...].astype(F32).T
    layer = bias_rows(layer_ref)
    no_cut = jnp.zeros((rows, channels), F32)
    place = lax.broadcasted_iota(jnp.int32, (TAIL, channels), 0)

    def neighbour(early, late):
        count = late.shape[0] - 8
        left, right = late[count : count + 1, :], late[count + 1 : count + 2, :]

        def tail(lanes):
            return jnp.where(place == TAIL - 1, left[:, lanes], jnp.where(place == 0, right[:, lanes], 0.0))

        flags = early[width:, :].T
        pieces = [jnp.broadcast_to(flags[:, k : k + 1], (channels, channels)) for k in range(width // channels)]
        mask = jnp.concatenate(pieces + [tail(slice(channels, None))], 0)
        x = jnp.concatenate([early[:width, :], tail(slice(0, channels))], 0)
        mixed = jnp.concatenate([late[:count, :channels], late[:count, channels:]], 0)
        return mask, split(x), mixed

    band = lax.axis_index("lat")
    even = lax.rem(band, 2) == 0
    masks, parts, mixed = zip(neighbour(early_first, late_first), neighbour(early_second, late_second))
    pair = hidden_pair(parts, mixed, (no_cut, no_cut), trig_ref[...], local_ref[...], layer, channels)
    one, two = (mask * y for mask, y in zip(masks, pair))
    above = jnp.where(band == 0, 0.0, jnp.where(even, two, one))
    below = jnp.where(band == bands - 1, 0.0, jnp.where(even, one, two))

    def at(row):
        return hidden_ref[row * block : (row + 1) * block, :]

    z = product([at(0), at(rows - 1)], filter_ref[4], channels)
    z = z + product([at(1), below], filter_ref[3], channels)
    z = z + product([above, at(rows - 2)], filter_ref[0], channels)
    copies = [middle]
    for r, row in enumerate((0, rows - 1)):
        t = columns(z[r * block : (r + 1) * block], channels, width)
        buf_ref[r] = (t + bias_ref[...]) * wet[:, row : row + 1]
        copy = pltpu.make_async_copy(buf_ref.at[pl.ds(r, 1)], out_ref.at[pl.ds(row, 1)], sem_ref.at[r])
        copy.start()
        copies.append(copy)
    for copy in copies:
        copy.wait()


def vmem():
    return pl.BlockSpec(memory_space=pltpu.VMEM)


def struct(shape, dtype=F32):
    return jax.ShapeDtypeStruct(shape, dtype)


def params(mib):
    return pltpu.CompilerParams(vmem_limit_bytes=mib * MIB)


def per_device(
    field, ocean, modes, spectral_weight, local_weight, layer_bias, conv_weight, conv_bias
):
    rows, width, channels = field.shape
    devices = lax.axis_size("lon")
    chips = devices // 2
    bands = lax.axis_size("lat")
    total_lon = width * devices
    total_modes = modes.shape[0]
    per = total_modes // devices
    half = chips * per
    block = width + TAIL
    steps = list(range(1, chips))
    wide = 2 * channels
    chunks = 2

    give, keep, away, early_first, early_second, high, low = pl.pallas_call(
        functools.partial(forward_kernel, chips, per, total_lon),
        out_shape=(
            struct((half + 1, rows, wide)),
            struct((half, rows, wide)),
            struct((1, rows, wide)),
            struct((width + 8, channels)),
            struct((width + 8, channels)),
            struct((rows, width, channels), BF16),
            struct((rows, width, channels), BF16),
        ),
        in_specs=[pl.BlockSpec(memory_space=pltpu.MemorySpace.HBM)] * 3,
        out_specs=(vmem(),) * 7,
        scratch_shapes=[
            pltpu.SMEM((total_modes,), jnp.int32),
            pltpu.VMEM((rows, width, channels), F32),
            pltpu.VMEM((rows, width), jnp.int32),
            pltpu.SemaphoreType.DMA((2,)),
            pltpu.SemaphoreType.DMA((chunks,)),
        ],
        compiler_params=params(16),
        name="forward",
    )(*[pltpu.with_memory_space_constraint(x, pltpu.MemorySpace.HBM) for x in (modes, field, ocean)])
    give = give.reshape((half + 1) * rows, wide)
    keep = keep.reshape(half * rows, wide)
    away = away.reshape(rows, wide)

    depth = -(-(6 * total_modes + rows + 8) // LANES) * LANES
    trig, local, mix = pl.pallas_call(
        functools.partial(prepare_kernel, chips, per, total_lon),
        out_shape=(
            struct((block, depth), BF16),
            struct((channels, 2 * channels), BF16),
            struct((per * wide, 2 * wide), BF16),
        ),
        in_specs=[vmem()] * 4,
        out_specs=(vmem(),) * 3,
        compiler_params=params(16),
        name="prepare",
    )(modes.reshape(1, total_modes), local_weight, spectral_weight, ocean)
    filters = pl.pallas_call(
        filter_kernel,
        out_shape=struct((5, 2 * channels, 6 * channels), BF16),
        in_specs=[vmem()],
        out_specs=vmem(),
        compiler_params=params(16),
        name="filters",
    )(conv_weight)

    got = lax.ppermute(give, "lon", pair_moves(chips))
    summed = keep + got[: half * rows]
    size = per * rows
    parts = {}
    for d in steps:
        send = summed[d * size : (d + 1) * size]
        if flip_of(d):
            send = jnp.concatenate([send, away])
        parts[d] = lax.ppermute(send, "lon", chip_moves(d, chips, flip_of(d)))
    crossed = [parts[d] for d in steps if flip_of(d)]
    evens = [(i, i + 1) for i in range(0, bands - 1, 2)]
    odds = [(i, i + 1) for i in range(1, bands - 1, 2)]
    if bands % 2 == 0 and bands > 2:
        odds.append((0, bands - 1))
    evens, odds = ([(a, b) for a, b in moves] + [(b, a) for a, b in moves] for moves in (evens, odds))
    early_first = lax.ppermute(early_first, "lat", evens)
    early_second = lax.ppermute(early_second, "lat", odds)

    own_mixed = pl.pallas_call(
        functools.partial(mix_kernel, per, rows),
        out_shape=struct((size, wide)),
        in_specs=[vmem()] * (len(steps) + 2),
        out_specs=vmem(),
        compiler_params=params(8),
        name="mix",
    )(summed, *[parts[d] for d in steps], mix)
    gathered = [own_mixed]
    for d in steps:
        gathered.append(lax.ppermute(own_mixed, "lon", chip_moves(d, chips, 0)))
    gathered = jnp.concatenate(gathered)
    other = lax.ppermute(gathered, "lon", pair_moves(chips))
    mixed = jnp.concatenate([gathered, other]).reshape(total_modes, rows, wide)

    late = struct((total_modes + 8, wide))
    late_first, late_second = pl.pallas_call(
        functools.partial(edges_kernel, chips, per),
        out_shape=(late, late),
        in_specs=[vmem()] * (2 + len(crossed)),
        out_specs=(vmem(),) * 2,
        compiler_params=params(8),
        name="edges",
    )(got, mixed, *crossed)
    late_first = lax.ppermute(late_first, "lat", evens)
    late_second = lax.ppermute(late_second, "lat", odds)
    layer = layer_bias.reshape(1, channels)
    hidden = pl.pallas_call(
        functools.partial(hidden_kernel, chips, per),
        out_shape=struct((rows * block, channels)),
        in_specs=[vmem()] * (7 + len(crossed)),
        out_specs=vmem(),
        compiler_params=params(24),
        cost_estimate=pl.CostEstimate(
            flops=6 * 256 * rows * width * channels, transcendentals=field.size, bytes_accessed=4 * field.size
        ),
        name="hidden",
    )(high, low, got, mixed, trig, local, layer, *crossed)

    bias = conv_bias.reshape(1, channels)
    firsts = list(range(1, rows - 1, 2))
    groups = [firsts[k : k + 2] for k in range(0, len(firsts), 2)]
    if len(groups) > 1 and len(groups[-1]) == 1:
        groups[-2:] = [groups[-2] + groups[-1]]
    flops = 2 * 6 * 4 * rows * width * channels * channels
    inner = pl.pallas_call(
        functools.partial(inner_kernel, groups),
        out_shape=struct((rows - 2, width, channels)),
        in_specs=[vmem()] * 4,
        out_specs=vmem(),
        compiler_params=params(24),
        cost_estimate=pl.CostEstimate(flops=flops, transcendentals=0, bytes_accessed=4 * field.size),
        name="inner",
    )(hidden, ocean, bias, filters)
    return pl.pallas_call(
        functools.partial(outer_kernel, bands),
        out_shape=struct((rows, width, channels)),
        in_specs=[vmem()] * 12,
        out_specs=pl.BlockSpec(memory_space=pl.ANY),
        scratch_shapes=[
            pltpu.VMEM((2, width, channels), F32),
            pltpu.SemaphoreType.DMA((3,)),
        ],
        compiler_params=params(24),
        name="outer",
    )(
        hidden, early_first, early_second, late_first, late_second, trig, local, layer, ocean, bias, filters, inner
    )


def solution(mesh):
    in_specs = (
        P("lat", "lon", None),
        P("lat", "lon"),
        P(),
        P("lon", None, None, None),
        P(),
        P(),
        P(),
        P(),
    )
    out_specs = P("lat", "lon", None)
    return jax.shard_map(
        per_device, mesh=mesh, in_specs=in_specs, out_specs=out_specs, check_vma=False
    )
```

```python
import functools
import math

import jax
import jax.numpy as jnp
from jax import lax
from jax.experimental import pallas as pl
from jax.experimental.pallas import tpu as pltpu
from jax.sharding import PartitionSpec as P

LANES = 128
TAIL = 8
MIB = 1 << 20
DRY = -(2.0**36)
F32 = jnp.float32
BF16 = jnp.bfloat16


def flip_of(distance):
    return 1 if distance & (distance + 1) == 0 and distance else 0


def chip_moves(distance, chips, flip):
    return [
        (2 * chip + core, 2 * (chip ^ distance) + (core ^ flip)) for chip in range(chips) for core in range(2)
    ]


def pair_moves(chips):
    return [(device, device ^ 1) for device in range(2 * chips)]


def split(x):
    high = x.astype(BF16)
    return high, (x - high.astype(F32)).astype(BF16)


def dot(a, b):
    return lax.dot_general(a, b, (((1,), (0,)), ((), ())), preferred_element_type=F32)


def fill(blocks, depth):
    missing = depth - sum(block.shape[0] for block in blocks)
    if missing:
        blocks = blocks + [jnp.zeros((missing,) + blocks[0].shape[1:], blocks[0].dtype)]
    return jnp.concatenate(blocks, 0)


def angles(mode_list, lon, total_lon):
    row = lax.broadcasted_iota(jnp.int32, lon.shape, 0)
    ids = jnp.zeros(lon.shape, jnp.int32)
    for index, mode in enumerate(mode_list):
        ids = jnp.where(row == index, mode, ids)
    return turns(ids * lon, total_lon)


def turns(product, total_lon):
    if total_lon & (total_lon - 1):
        product = lax.rem(product, total_lon)
    else:
        product = product & (total_lon - 1)
    return product.astype(F32) * (2.0 * math.pi / total_lon)


def forward_kernel(
    chips, per, total_lon, modes_hbm, field_hbm, ocean_hbm, give_ref, keep_ref, away_ref, first_ref, second_ref,
    high_ref, low_ref,     modes_ref, field_ref, ocean_ref, small_sem, field_sem,
):
    rows, width, channels = field_ref.shape
    chunks = field_sem.shape[0]
    step = rows // chunks
    first_copy = pltpu.make_async_copy(modes_hbm, modes_ref, small_sem.at[0])
    first_copy.start()
    copies = []
    for k in range(chunks):
        part = pl.ds(k * step, step)
        copies.append(pltpu.make_async_copy(field_hbm.at[part], field_ref.at[part], field_sem.at[k]))
        copies[-1].start()
    ocean_copy = pltpu.make_async_copy(ocean_hbm, ocean_ref, small_sem.at[1])
    ocean_copy.start()
    here = lax.axis_index("lon")
    chip, core = here // 2, lax.rem(here, 2)
    first_copy.wait()
    mode_list = []
    for flipped in range(2):
        for d in range(chips):
            owner = 2 * (chip ^ d) + lax.rem(core + flipped + flip_of(d), 2)
            mode_list += [modes_ref[owner * per + t] for t in range(per)]
    count = len(mode_list)
    half = count // 2
    lon = here * width + lax.broadcasted_iota(jnp.int32, (count, width), 1)
    theta = angles(mode_list, lon, total_lon)
    scale = 1.0 / math.sqrt(total_lon)
    table = jnp.concatenate([jnp.cos(theta) * scale, -jnp.sin(theta) * scale], 0)
    lhs = jnp.concatenate(split(table), 0)
    for i in range(rows):
        if i % step == 0:
            copies[i // step].wait()
        high, low = split(field_ref[i])
        high_ref[i] = high
        low_ref[i] = low
        product = dot(lhs, jnp.concatenate([high, low], 1))
        total = product[: 2 * count] + product[2 * count :]
        total = total[:, :channels] + total[:, channels:]
        keep_ref[:half, i, :channels] = total[:half]
        give_ref[:half, i, :channels] = total[half:count]
        keep_ref[:half, i, channels:] = total[count : count + half]
        give_ref[:half, i, channels:] = total[count + half :]
    ocean_copy.wait()
    last = field_ref[:, width - 1, :]
    first = field_ref[:, 0, :]
    land = ocean_ref[...].astype(F32)
    last_wet = jnp.broadcast_to(land[:, width - 1 : width], (rows, channels))
    first_wet = jnp.broadcast_to(land[:, :1], (rows, channels))
    even = lax.rem(lax.axis_index("lat"), 2) == 0
    for out, at_end in ((first_ref, even), (second_ref, ~even)):
        out[:width, :] = jnp.where(at_end, field_ref[rows - 1], field_ref[0])
        row = jnp.where(at_end, land[rows - 1 :], land[:1])
        pieces = [row[:, k : k + channels] for k in range(0, width, channels)]
        out[width:, :] = fill(pieces, out.shape[0] - width)
    near_is_last = core == 0
    give_ref[half, :, :channels] = jnp.where(near_is_last, last, first)
    give_ref[half, :, channels:] = jnp.where(near_is_last, last_wet, first_wet)
    away_ref[0, :, :channels] = jnp.where(near_is_last, first, last)
    away_ref[0, :, channels:] = jnp.where(near_is_last, first_wet, last_wet)


def prepare_kernel(
    chips, per, total_lon, modes_ref, local_ref, spectral_ref, ocean_ref, trig_ref, local_out, mix_ref
):
    channels = local_ref.shape[0]
    rows, width = ocean_ref.shape
    wide = 2 * channels
    for t in range(per):
        real, imag = spectral_ref[t, 0], spectral_ref[t, 1]
        top = jnp.concatenate(split(jnp.concatenate([real, imag], 1)), 1)
        low = jnp.concatenate(split(jnp.concatenate([-imag, real], 1)), 1)
        mix_ref[t * wide : t * wide + channels, :] = top
        mix_ref[t * wide + channels : (t + 1) * wide, :] = low
    here = lax.axis_index("lon")
    chip, core = here // 2, lax.rem(here, 2)
    count = modes_ref.shape[1]
    spot = lax.broadcasted_iota(jnp.int32, (count, count), 0)
    slot = lax.div(spot, per)
    flipped, d = lax.div(slot, chips), lax.rem(slot, chips)
    source = 2 * (chip ^ d) + (core ^ flipped)
    wanted = source * per + lax.rem(spot, per)
    hit = wanted == lax.broadcasted_iota(jnp.int32, (count, count), 1)
    mine = jnp.sum(jnp.where(hit, modes_ref[...].astype(F32), 0.0), 1, keepdims=True).astype(jnp.int32)
    block = width + TAIL
    padded = -(-block // LANES) * LANES
    place = lax.broadcasted_iota(jnp.int32, (count, padded), 1)
    place = jnp.where(place == block - 1, -1, place)
    lon = here * width + place + total_lon
    lon = jnp.where(lon >= total_lon, lon - total_lon, lon)
    lon = jnp.where(lon >= total_lon, lon - total_lon, lon)
    theta = turns(mine * lon, total_lon)
    scale = 2.0 / math.sqrt(count)
    table = jnp.concatenate([jnp.cos(theta) * scale, -jnp.sin(theta) * scale], 0)
    high, low = split(table)
    high, low = high.astype(F32), low.astype(F32)
    land = 1.0 - ocean_ref[...].astype(F32)
    land = jnp.concatenate([land, jnp.ones((rows, padded - width), F32)], 1)
    ones = jnp.where(lax.broadcasted_iota(jnp.int32, (8, padded), 0) < 3, 1.0, 0.0)
    stacked = fill([high, low, high, land, ones], trig_ref.shape[1])
    trig_ref[...] = stacked.T[:block].astype(BF16)
    local_out[...] = jnp.concatenate(split(local_ref[...]), 1)


def filter_kernel(conv_ref, out_ref):
    channels = conv_ref.shape[2]
    for col in range(3):
        left = slice(col * channels, (col + 1) * channels)
        right = slice((3 + col) * channels, (4 + col) * channels)
        low, mid, up = (0.5 * conv_ref[row, col] for row in range(3))
        outer = 0.5 * (low + up)
        even4, even6 = (low + 4.0 * up) * (1.0 / 24.0), (low + up) * (-1.0 / 6.0)
        odd4, odd6 = mid * (1.0 / 12.0), mid * (1.0 / 6.0)
        quads = (0.25 * low, even6 - odd6, even6 + odd6, even4 + odd4, even4 - odd4, up)
        pairs = (low, outer + 0.5 * mid, outer - 0.5 * mid, up, mid)
        for k, taps in enumerate(pairs + quads[:-1]):
            top, bottom = split(taps)
            out_ref[k, :channels, left] = top
            out_ref[k, :channels, right] = bottom
            out_ref[k, channels:, left] = top
            out_ref[k, channels:, right] = jnp.zeros_like(top)


def twice_gelu(x):
    slope = math.sqrt(2.0 / math.pi)
    return x * (1.0 + jnp.tanh(x * (slope + (slope * 0.044715) * (x * x))))


def hidden_pair(parts, mixed, cuts, trig, local, bias, channels):
    depth = trig.shape[1]
    top = local[:, :channels]
    none = jnp.zeros_like(top)
    both = jnp.concatenate([jnp.concatenate([top, none], 1), jnp.concatenate([none, top], 1)], 0)
    rest = dot(jnp.concatenate([parts[0][1], parts[1][1]], 1), both)
    out = []
    for r in range(2):
        m_high, m_low = split(mixed[r])
        lower = fill([m_high, m_high, m_low, jnp.concatenate([cuts[r], bias], 0).astype(BF16)], depth)
        rhs = jnp.concatenate([lower, jnp.zeros((depth, channels), BF16)], 1)
        y = dot(jnp.concatenate([parts[r][0], trig], 1), jnp.concatenate([local, rhs], 0))
        out.append(twice_gelu(y[:, :channels] + y[:, channels:] + rest[:, r * channels : (r + 1) * channels]))
    return out


def bias_rows(bias_ref):
    high, mid = split(bias_ref[...])
    high, mid = high.astype(F32), mid.astype(F32)
    row = lax.broadcasted_iota(jnp.int32, (8, high.shape[1]), 0)
    rest = jnp.where(row == 2, bias_ref[...] - high - mid, 0.0)
    return jnp.where(row == 0, high, jnp.where(row == 1, mid, rest))


def side_columns(chips, per, rows, got_ref, far_refs):
    here = lax.axis_index("lon")
    chip, south = here // 2, lax.rem(here, 2) == 0
    other = lax.rem(jnp.where(south, chip + chips - 1, chip + 1), chips)
    far = far_refs[0][per * rows :, :]
    masks = [d for d in range(chips) if flip_of(d)]
    for d, ref in zip(masks[1:], far_refs[1:]):
        far = jnp.where((chip ^ other) == d, ref[per * rows :, :], far)
    near = got_ref[got_ref.shape[0] - rows :, :]
    return jnp.where(south, far, near), jnp.where(south, near, far)


def edges_kernel(chips, per, got_ref, mixed_ref, *refs):
    *far_refs, first_ref, second_ref = refs
    count, rows, _ = mixed_ref.shape
    left, right = side_columns(chips, per, rows, got_ref, far_refs)
    even = lax.rem(lax.axis_index("lat"), 2) == 0
    for out, at_end in ((first_ref, even), (second_ref, ~even)):
        out[:count, :] = jnp.where(at_end, mixed_ref[:, rows - 1, :], mixed_ref[:, 0, :])
        sides = [jnp.where(at_end, side[rows - 1 :], side[:1]) for side in (left, right)]
        out[count:, :] = fill(sides, out.shape[0] - count)


def mix_kernel(per, rows, *refs):
    summed_ref, *part_refs, mix_ref, out_ref = refs
    wide = summed_ref.shape[1]
    for t in range(per):
        at = slice(t * rows, (t + 1) * rows)
        total = summed_ref[at, :]
        for part in part_refs:
            total = total + part[at, :]
        high, low = split(total)
        weights = mix_ref[t * wide : (t + 1) * wide, :]
        y = dot(high, weights)
        out_ref[at, :] = y[:, :wide] + y[:, wide:] + dot(low, weights[:, :wide])


def hidden_kernel(chips, per, high_ref, low_ref, got_ref, mixed_ref, trig_ref, local_ref, bias_ref, *refs):
    *far_refs, hidden_ref = refs
    rows, width, channels = high_ref.shape
    block = width + TAIL
    count = mixed_ref.shape[0]
    depth = trig_ref.shape[1]
    local = local_ref[...]
    left, right = side_columns(chips, per, rows, got_ref, far_refs)
    place = lax.broadcasted_iota(jnp.int32, (TAIL, channels), 0)
    first = 6 * count
    lane = lax.broadcasted_iota(jnp.int32, (rows, depth), 1)
    mine = lane == first + lax.broadcasted_iota(jnp.int32, (rows, depth), 0)
    dry = [
        jnp.sum(jnp.where(mine, 1.0 - side[:, channels : channels + 1], 0.0), 0, keepdims=True)
        for side in (left, right)
    ]
    tail_place = lax.broadcasted_iota(jnp.int32, (TAIL, depth), 0)
    tail_lane = lax.broadcasted_iota(jnp.int32, (TAIL, depth), 1)
    is_land = (tail_lane >= first) & (tail_lane < first + rows)
    end = trig_ref[width:, :].astype(F32)
    end = jnp.where(is_land & (tail_place == TAIL - 1), dry[0], end)
    end = jnp.where(is_land & (tail_place == 0), dry[1], end)
    trig = jnp.concatenate([trig_ref[:width, :], end.astype(BF16)], 0)
    bias = bias_rows(bias_ref)
    select = lax.broadcasted_iota(jnp.int32, (rows, channels), 0)
    for i in range(0, rows, 2):
        parts, mixed, cuts = [], [], []
        for r in (i, i + 1):
            side = jnp.where(
                place == TAIL - 1, left[r : r + 1, :channels], jnp.where(place == 0, right[r : r + 1, :channels], 0.0)
            )
            high, low = split(side)
            parts.append((jnp.concatenate([high_ref[r], high], 0), jnp.concatenate([low_ref[r], low], 0)))
            mixed.append(jnp.concatenate([mixed_ref[:, r, :channels], mixed_ref[:, r, channels:]], 0))
            cuts.append(jnp.where(select == r, DRY, 0.0))
        pair = hidden_pair(parts, mixed, cuts, trig, local, bias, channels)
        for r in range(2):
            hidden_ref[(i + r) * block : (i + r + 1) * block, :] = pair[r]


def columns(t, channels, keep):
    west = pltpu.roll(t[:, :channels], 1, 0)
    east = pltpu.roll(t[:, 2 * channels :], t.shape[0] - 1, 0)
    return (west + t[:, channels : 2 * channels] + east)[:keep]


def product(parts, weights, channels):
    y = dot(jnp.concatenate(split(jnp.concatenate(parts, 0)), 1), weights)
    return y[:, : 3 * channels] + y[:, 3 * channels :]


def inner_kernel(groups, hidden_ref, ocean_ref, bias_ref, filter_ref, out_ref):
    _, width = ocean_ref.shape
    channels = hidden_ref.shape[1]
    block = width + TAIL
    wet = ocean_ref[...].astype(F32).T

    def rows_of(first, count):
        return [hidden_ref[(first - 1 + k) * block : (first + k) * block, :] for k in range(count)]

    def write(sums, firsts):
        for g, first in enumerate(firsts):
            for r, t in enumerate(sums):
                t = columns(t[g * block : (g + 1) * block], channels, width)
                row = first + r
                out_ref[row - 1] = (t + bias_ref[...]) * wet[:, row : row + 1]

    quads, pairs = groups
    if quads:
        terms = [[] for _ in range(6)]
        for first in quads:
            d = rows_of(first, 6)
            a, b = d[4] - 4.0 * d[2], d[3] - 4.0 * d[1]
            p, q = d[4] - d[2], 2.0 * (d[3] - d[1])
            for k, term in enumerate(
                (4.0 * d[0] - 5.0 * d[2] + d[4], a + b, a - b, p + q, p - q, 4.0 * d[1] - 5.0 * d[3] + d[5])
            ):
                terms[k].append(term)
        m = [product(terms[k], filter_ref[index], channels) for k, index in enumerate((5, 6, 7, 8, 9, 3))]
        sum1, dif1, sum2, dif2 = m[1] + m[2], m[1] - m[2], m[3] + m[4], m[3] - m[4]
        write((m[0] + sum1 + sum2, dif1 + 2.0 * dif2, sum1 + 4.0 * sum2, dif1 + 8.0 * dif2 + m[5]), quads)
    if pairs:
        terms = [[] for _ in range(4)]
        for first in pairs:
            d = rows_of(first, 4)
            for k, term in enumerate((d[0] - d[2], d[1] + d[2], d[2] - d[1], d[1] - d[3])):
                terms[k].append(term)
        m = [product(terms[k], filter_ref[k], channels) for k in range(4)]
        write((m[0] + m[1] + m[2], m[1] - m[2] - m[3]), pairs)


def outer_kernel(
    bands, hidden_ref, early_first, early_second, late_first, late_second, trig_ref, local_ref, layer_ref,
    ocean_ref, bias_ref, filter_ref, inner_ref, out_ref, buf_ref, sem_ref,
):
    rows, width = ocean_ref.shape
    channels = local_ref.shape[0]
    block = width + TAIL
    middle = pltpu.make_async_copy(inner_ref, out_ref.at[pl.ds(1, rows - 2)], sem_ref.at[2])
    middle.start()
    wet = ocean_ref[...].astype(F32).T
    layer = bias_rows(layer_ref)
    no_cut = jnp.zeros((rows, channels), F32)
    place = lax.broadcasted_iota(jnp.int32, (TAIL, channels), 0)

    def neighbour(early, late):
        count = late.shape[0] - 8
        left, right = late[count : count + 1, :], late[count + 1 : count + 2, :]

        def tail(lanes):
            return jnp.where(place == TAIL - 1, left[:, lanes], jnp.where(place == 0, right[:, lanes], 0.0))

        flags = early[width:, :].T
        pieces = [jnp.broadcast_to(flags[:, k : k + 1], (channels, channels)) for k in range(width // channels)]
        mask = jnp.concatenate(pieces + [tail(slice(channels, None))], 0)
        x = jnp.concatenate([early[:width, :], tail(slice(0, channels))], 0)
        mixed = jnp.concatenate([late[:count, :channels], late[:count, channels:]], 0)
        return mask, split(x), mixed

    band = lax.axis_index("lat")
    even = lax.rem(band, 2) == 0
    masks, parts, mixed = zip(neighbour(early_first, late_first), neighbour(early_second, late_second))
    pair = hidden_pair(parts, mixed, (no_cut, no_cut), trig_ref[...], local_ref[...], layer, channels)
    one, two = (mask * y for mask, y in zip(masks, pair))
    above = jnp.where(band == 0, 0.0, jnp.where(even, two, one))
    below = jnp.where(band == bands - 1, 0.0, jnp.where(even, one, two))

    def at(row):
        return hidden_ref[row * block : (row + 1) * block, :]

    z = product([at(0), at(rows - 1)], filter_ref[4], channels)
    z = z + product([at(1), below], filter_ref[3], channels)
    z = z + product([above, at(rows - 2)], filter_ref[0], channels)
    copies = [middle]
    for r, row in enumerate((0, rows - 1)):
        t = columns(z[r * block : (r + 1) * block], channels, width)
        buf_ref[r] = (t + bias_ref[...]) * wet[:, row : row + 1]
        copy = pltpu.make_async_copy(buf_ref.at[pl.ds(r, 1)], out_ref.at[pl.ds(row, 1)], sem_ref.at[r])
        copy.start()
        copies.append(copy)
    for copy in copies:
        copy.wait()


def vmem():
    return pl.BlockSpec(memory_space=pltpu.VMEM)


def struct(shape, dtype=F32):
    return jax.ShapeDtypeStruct(shape, dtype)


def params(mib):
    return pltpu.CompilerParams(vmem_limit_bytes=mib * MIB)


def per_device(
    field, ocean, modes, spectral_weight, local_weight, layer_bias, conv_weight, conv_bias
):
    rows, width, channels = field.shape
    devices = lax.axis_size("lon")
    chips = devices // 2
    bands = lax.axis_size("lat")
    total_lon = width * devices
    total_modes = modes.shape[0]
    per = total_modes // devices
    half = chips * per
    block = width + TAIL
    steps = list(range(1, chips))
    wide = 2 * channels
    chunks = 2

    give, keep, away, early_first, early_second, high, low = pl.pallas_call(
        functools.partial(forward_kernel, chips, per, total_lon),
        out_shape=(
            struct((half + 1, rows, wide)),
            struct((half, rows, wide)),
            struct((1, rows, wide)),
            struct((width + 8, channels)),
            struct((width + 8, channels)),
            struct((rows, width, channels), BF16),
            struct((rows, width, channels), BF16),
        ),
        in_specs=[pl.BlockSpec(memory_space=pltpu.MemorySpace.HBM)] * 3,
        out_specs=(vmem(),) * 7,
        scratch_shapes=[
            pltpu.SMEM((total_modes,), jnp.int32),
            pltpu.VMEM((rows, width, channels), F32),
            pltpu.VMEM((rows, width), jnp.int32),
            pltpu.SemaphoreType.DMA((2,)),
            pltpu.SemaphoreType.DMA((chunks,)),
        ],
        compiler_params=params(16),
        name="forward",
    )(*[pltpu.with_memory_space_constraint(x, pltpu.MemorySpace.HBM) for x in (modes, field, ocean)])
    give = give.reshape((half + 1) * rows, wide)
    keep = keep.reshape(half * rows, wide)
    away = away.reshape(rows, wide)

    depth = -(-(6 * total_modes + rows + 8) // LANES) * LANES
    trig, local, mix = pl.pallas_call(
        functools.partial(prepare_kernel, chips, per, total_lon),
        out_shape=(
            struct((block, depth), BF16),
            struct((channels, 2 * channels), BF16),
            struct((per * wide, 2 * wide), BF16),
        ),
        in_specs=[vmem()] * 4,
        out_specs=(vmem(),) * 3,
        compiler_params=params(16),
        name="prepare",
    )(modes.reshape(1, total_modes), local_weight, spectral_weight, ocean)
    filters = pl.pallas_call(
        filter_kernel,
        out_shape=struct((10, 2 * channels, 6 * channels), BF16),
        in_specs=[vmem()],
        out_specs=vmem(),
        compiler_params=params(16),
        name="filters",
    )(conv_weight)

    got = lax.ppermute(give, "lon", pair_moves(chips))
    summed = keep + got[: half * rows]
    size = per * rows
    parts = {}
    for d in steps:
        send = summed[d * size : (d + 1) * size]
        if flip_of(d):
            send = jnp.concatenate([send, away])
        parts[d] = lax.ppermute(send, "lon", chip_moves(d, chips, flip_of(d)))
    crossed = [parts[d] for d in steps if flip_of(d)]
    evens = [(i, i + 1) for i in range(0, bands - 1, 2)]
    odds = [(i, i + 1) for i in range(1, bands - 1, 2)]
    if bands % 2 == 0 and bands > 2:
        odds.append((0, bands - 1))
    evens, odds = ([(a, b) for a, b in moves] + [(b, a) for a, b in moves] for moves in (evens, odds))
    early_first = lax.ppermute(early_first, "lat", evens)
    early_second = lax.ppermute(early_second, "lat", odds)

    own_mixed = pl.pallas_call(
        functools.partial(mix_kernel, per, rows),
        out_shape=struct((size, wide)),
        in_specs=[vmem()] * (len(steps) + 2),
        out_specs=vmem(),
        compiler_params=params(8),
        name="mix",
    )(summed, *[parts[d] for d in steps], mix)
    gathered = [own_mixed]
    for d in steps:
        gathered.append(lax.ppermute(own_mixed, "lon", chip_moves(d, chips, 0)))
    gathered = jnp.concatenate(gathered)
    other = lax.ppermute(gathered, "lon", pair_moves(chips))
    mixed = jnp.concatenate([gathered, other]).reshape(total_modes, rows, wide)

    late = struct((total_modes + 8, wide))
    late_first, late_second = pl.pallas_call(
        functools.partial(edges_kernel, chips, per),
        out_shape=(late, late),
        in_specs=[vmem()] * (2 + len(crossed)),
        out_specs=(vmem(),) * 2,
        compiler_params=params(8),
        name="edges",
    )(got, mixed, *crossed)
    late_first = lax.ppermute(late_first, "lat", evens)
    late_second = lax.ppermute(late_second, "lat", odds)
    layer = layer_bias.reshape(1, channels)
    hidden = pl.pallas_call(
        functools.partial(hidden_kernel, chips, per),
        out_shape=struct((rows * block, channels)),
        in_specs=[vmem()] * (7 + len(crossed)),
        out_specs=vmem(),
        compiler_params=params(24),
        cost_estimate=pl.CostEstimate(
            flops=6 * 256 * rows * width * channels, transcendentals=field.size, bytes_accessed=4 * field.size
        ),
        name="hidden",
    )(high, low, got, mixed, trig, local, layer, *crossed)

    bias = conv_bias.reshape(1, channels)
    whole = (rows - 2) // 4 * 4
    groups = (list(range(1, whole, 4)), list(range(1 + whole, rows - 1, 2)))
    flops = 2 * 6 * 4 * rows * width * channels * channels
    inner = pl.pallas_call(
        functools.partial(inner_kernel, groups),
        out_shape=struct((rows - 2, width, channels)),
        in_specs=[vmem()] * 4,
        out_specs=vmem(),
        compiler_params=params(24),
        cost_estimate=pl.CostEstimate(flops=flops, transcendentals=0, bytes_accessed=4 * field.size),
        name="inner",
    )(hidden, ocean, bias, filters)
    return pl.pallas_call(
        functools.partial(outer_kernel, bands),
        out_shape=struct((rows, width, channels)),
        in_specs=[vmem()] * 12,
        out_specs=pl.BlockSpec(memory_space=pl.ANY),
        scratch_shapes=[
            pltpu.VMEM((2, width, channels), F32),
            pltpu.SemaphoreType.DMA((3,)),
        ],
        compiler_params=params(24),
        name="outer",
    )(
        hidden, early_first, early_second, late_first, late_second, trig, local, layer, ocean, bias, filters, inner
    )


def solution(mesh):
    in_specs = (
        P("lat", "lon", None),
        P("lat", "lon"),
        P(),
        P("lon", None, None, None),
        P(),
        P(),
        P(),
        P(),
    )
    out_specs = P("lat", "lon", None)
    return jax.shard_map(
        per_device, mesh=mesh, in_specs=in_specs, out_specs=out_specs, check_vma=False
    )
```

```python
import functools
import math

import jax
import jax.numpy as jnp
from jax import lax
from jax.experimental import pallas as pl
from jax.experimental.pallas import tpu as pltpu
from jax.sharding import PartitionSpec as P

LANES = 128
TAIL = 8
MIB = 1 << 20
DRY = -(2.0**36)
F32 = jnp.float32
BF16 = jnp.bfloat16


def flip_of(distance):
    return 1 if distance & (distance + 1) == 0 and distance else 0


def chip_moves(distance, chips, flip):
    return [
        (2 * chip + core, 2 * (chip ^ distance) + (core ^ flip)) for chip in range(chips) for core in range(2)
    ]


def pair_moves(chips):
    return [(device, device ^ 1) for device in range(2 * chips)]


def split(x):
    high = x.astype(BF16)
    return high, (x - high.astype(F32)).astype(BF16)


def dot(a, b):
    return lax.dot_general(a, b, (((1,), (0,)), ((), ())), preferred_element_type=F32)


def fill(blocks, depth):
    missing = depth - sum(block.shape[0] for block in blocks)
    if missing:
        blocks = blocks + [jnp.zeros((missing,) + blocks[0].shape[1:], blocks[0].dtype)]
    return jnp.concatenate(blocks, 0)


def angles(mode_list, lon, total_lon):
    row = lax.broadcasted_iota(jnp.int32, lon.shape, 0)
    ids = jnp.zeros(lon.shape, jnp.int32)
    for index, mode in enumerate(mode_list):
        ids = jnp.where(row == index, mode, ids)
    return turns(ids * lon, total_lon)


def turns(product, total_lon):
    if total_lon & (total_lon - 1):
        product = lax.rem(product, total_lon)
    else:
        product = product & (total_lon - 1)
    return product.astype(F32) * (2.0 * math.pi / total_lon)


def forward_kernel(
    chips, per, total_lon, modes_hbm, field_hbm, ocean_hbm, give_ref, keep_ref, away_ref, first_ref, second_ref,
    high_ref, low_ref,     modes_ref, field_ref, ocean_ref, small_sem, field_sem,
):
    rows, width, channels = field_ref.shape
    starts = [0, rows * 3 // 4]
    first_copy = pltpu.make_async_copy(modes_hbm, modes_ref, small_sem.at[0])
    first_copy.start()
    copies = []
    for k, (start, stop) in enumerate(zip(starts, starts[1:] + [rows])):
        part = pl.ds(start, stop - start)
        copies.append(pltpu.make_async_copy(field_hbm.at[part], field_ref.at[part], field_sem.at[k]))
        copies[-1].start()
    ocean_copy = pltpu.make_async_copy(ocean_hbm, ocean_ref, small_sem.at[1])
    ocean_copy.start()
    here = lax.axis_index("lon")
    chip, core = here // 2, lax.rem(here, 2)
    first_copy.wait()
    mode_list = []
    for flipped in range(2):
        for d in range(chips):
            owner = 2 * (chip ^ d) + lax.rem(core + flipped + flip_of(d), 2)
            mode_list += [modes_ref[owner * per + t] for t in range(per)]
    count = len(mode_list)
    half = count // 2
    lon = here * width + lax.broadcasted_iota(jnp.int32, (count, width), 1)
    theta = angles(mode_list, lon, total_lon)
    scale = 1.0 / math.sqrt(total_lon)
    table = jnp.concatenate([jnp.cos(theta) * scale, -jnp.sin(theta) * scale], 0)
    lhs = jnp.concatenate(split(table), 0)
    for i in range(rows):
        if i in starts:
            copies[starts.index(i)].wait()
        high, low = split(field_ref[i])
        high_ref[i] = high
        low_ref[i] = low
        product = dot(lhs, jnp.concatenate([high, low], 1))
        total = product[: 2 * count] + product[2 * count :]
        total = total[:, :channels] + total[:, channels:]
        keep_ref[:half, i, :channels] = total[:half]
        give_ref[:half, i, :channels] = total[half:count]
        keep_ref[:half, i, channels:] = total[count : count + half]
        give_ref[:half, i, channels:] = total[count + half :]
    ocean_copy.wait()
    last = field_ref[:, width - 1, :]
    first = field_ref[:, 0, :]
    land = ocean_ref[...].astype(F32)
    last_wet = jnp.broadcast_to(land[:, width - 1 : width], (rows, channels))
    first_wet = jnp.broadcast_to(land[:, :1], (rows, channels))
    even = lax.rem(lax.axis_index("lat"), 2) == 0
    for out, at_end in ((first_ref, even), (second_ref, ~even)):
        out[:width, :] = jnp.where(at_end, field_ref[rows - 1], field_ref[0])
        row = jnp.where(at_end, land[rows - 1 :], land[:1])
        pieces = [row[:, k : k + channels] for k in range(0, width, channels)]
        out[width:, :] = fill(pieces, out.shape[0] - width)
    near_is_last = core == 0
    give_ref[half, :, :channels] = jnp.where(near_is_last, last, first)
    give_ref[half, :, channels:] = jnp.where(near_is_last, last_wet, first_wet)
    away_ref[0, :, :channels] = jnp.where(near_is_last, first, last)
    away_ref[0, :, channels:] = jnp.where(near_is_last, first_wet, last_wet)


def prepare_kernel(
    chips, per, total_lon, modes_ref, local_ref, spectral_ref, ocean_ref, trig_ref, local_out, mix_ref
):
    channels = local_ref.shape[0]
    rows, width = ocean_ref.shape
    wide = 2 * channels
    for t in range(per):
        real, imag = spectral_ref[t, 0], spectral_ref[t, 1]
        top = jnp.concatenate(split(jnp.concatenate([real, imag], 1)), 1)
        low = jnp.concatenate(split(jnp.concatenate([-imag, real], 1)), 1)
        mix_ref[t * wide : t * wide + channels, :] = top
        mix_ref[t * wide + channels : (t + 1) * wide, :] = low
    here = lax.axis_index("lon")
    chip, core = here // 2, lax.rem(here, 2)
    count = modes_ref.shape[1]
    spot = lax.broadcasted_iota(jnp.int32, (count, count), 0)
    slot = lax.div(spot, per)
    flipped, d = lax.div(slot, chips), lax.rem(slot, chips)
    source = 2 * (chip ^ d) + (core ^ flipped)
    wanted = source * per + lax.rem(spot, per)
    hit = wanted == lax.broadcasted_iota(jnp.int32, (count, count), 1)
    mine = jnp.sum(jnp.where(hit, modes_ref[...].astype(F32), 0.0), 1, keepdims=True).astype(jnp.int32)
    block = width + TAIL
    padded = -(-block // LANES) * LANES
    place = lax.broadcasted_iota(jnp.int32, (count, padded), 1)
    place = jnp.where(place == block - 1, -1, place)
    lon = here * width + place + total_lon
    lon = jnp.where(lon >= total_lon, lon - total_lon, lon)
    lon = jnp.where(lon >= total_lon, lon - total_lon, lon)
    theta = turns(mine * lon, total_lon)
    scale = 2.0 / math.sqrt(count)
    table = jnp.concatenate([jnp.cos(theta) * scale, -jnp.sin(theta) * scale], 0)
    high, low = split(table)
    high, low = high.astype(F32), low.astype(F32)
    land = 1.0 - ocean_ref[...].astype(F32)
    land = jnp.concatenate([land, jnp.ones((rows, padded - width), F32)], 1)
    ones = jnp.where(lax.broadcasted_iota(jnp.int32, (8, padded), 0) < 3, 1.0, 0.0)
    stacked = fill([high, low, high, land, ones], trig_ref.shape[1])
    trig_ref[...] = stacked.T[:block].astype(BF16)
    local_out[...] = jnp.concatenate(split(local_ref[...]), 1)


def filter_kernel(conv_ref, out_ref):
    channels = conv_ref.shape[2]
    for col in range(3):
        left = slice(col * channels, (col + 1) * channels)
        right = slice((3 + col) * channels, (4 + col) * channels)
        low, mid, up = (0.5 * conv_ref[row, col] for row in range(3))
        outer = 0.5 * (low + up)
        even4, even6 = (low + 4.0 * up) * (1.0 / 24.0), (low + up) * (-1.0 / 6.0)
        odd4, odd6 = mid * (1.0 / 12.0), mid * (1.0 / 6.0)
        quads = (0.25 * low, even6 - odd6, even6 + odd6, even4 + odd4, even4 - odd4, up)
        pairs = (low, outer + 0.5 * mid, outer - 0.5 * mid, up, mid)
        for k, taps in enumerate(pairs + quads[:-1]):
            top, bottom = split(taps)
            out_ref[k, :channels, left] = top
            out_ref[k, :channels, right] = bottom
            out_ref[k, channels:, left] = top
            out_ref[k, channels:, right] = jnp.zeros_like(top)


def twice_gelu(x):
    slope = math.sqrt(2.0 / math.pi)
    return x * (1.0 + jnp.tanh(x * (slope + (slope * 0.044715) * (x * x))))


def hidden_pair(parts, mixed, cuts, trig, local, bias, channels):
    depth = trig.shape[1]
    top = local[:, :channels]
    none = jnp.zeros_like(top)
    both = jnp.concatenate([jnp.concatenate([top, none], 1), jnp.concatenate([none, top], 1)], 0)
    rest = dot(jnp.concatenate([parts[0][1], parts[1][1]], 1), both)
    out = []
    for r in range(2):
        m_high, m_low = split(mixed[r])
        lower = fill([m_high, m_high, m_low, jnp.concatenate([cuts[r], bias], 0).astype(BF16)], depth)
        rhs = jnp.concatenate([lower, jnp.zeros((depth, channels), BF16)], 1)
        y = dot(jnp.concatenate([parts[r][0], trig], 1), jnp.concatenate([local, rhs], 0))
        out.append(twice_gelu(y[:, :channels] + y[:, channels:] + rest[:, r * channels : (r + 1) * channels]))
    return out


def bias_rows(bias_ref):
    high, mid = split(bias_ref[...])
    high, mid = high.astype(F32), mid.astype(F32)
    row = lax.broadcasted_iota(jnp.int32, (8, high.shape[1]), 0)
    rest = jnp.where(row == 2, bias_ref[...] - high - mid, 0.0)
    return jnp.where(row == 0, high, jnp.where(row == 1, mid, rest))


def side_columns(chips, per, rows, got_ref, far_refs):
    here = lax.axis_index("lon")
    chip, south = here // 2, lax.rem(here, 2) == 0
    other = lax.rem(jnp.where(south, chip + chips - 1, chip + 1), chips)
    far = far_refs[0][per * rows :, :]
    masks = [d for d in range(chips) if flip_of(d)]
    for d, ref in zip(masks[1:], far_refs[1:]):
        far = jnp.where((chip ^ other) == d, ref[per * rows :, :], far)
    near = got_ref[got_ref.shape[0] - rows :, :]
    return jnp.where(south, far, near), jnp.where(south, near, far)


def edges_kernel(chips, per, got_ref, mixed_ref, *refs):
    *far_refs, first_ref, second_ref = refs
    count, rows, _ = mixed_ref.shape
    left, right = side_columns(chips, per, rows, got_ref, far_refs)
    even = lax.rem(lax.axis_index("lat"), 2) == 0
    for out, at_end in ((first_ref, even), (second_ref, ~even)):
        out[:count, :] = jnp.where(at_end, mixed_ref[:, rows - 1, :], mixed_ref[:, 0, :])
        sides = [jnp.where(at_end, side[rows - 1 :], side[:1]) for side in (left, right)]
        out[count:, :] = fill(sides, out.shape[0] - count)


def mix_kernel(per, rows, *refs):
    summed_ref, *part_refs, mix_ref, out_ref = refs
    wide = summed_ref.shape[1]
    for t in range(per):
        at = slice(t * rows, (t + 1) * rows)
        total = summed_ref[at, :]
        for part in part_refs:
            total = total + part[at, :]
        high, low = split(total)
        weights = mix_ref[t * wide : (t + 1) * wide, :]
        y = dot(high, weights)
        out_ref[at, :] = y[:, :wide] + y[:, wide:] + dot(low, weights[:, :wide])


def hidden_kernel(chips, per, high_ref, low_ref, got_ref, mixed_ref, trig_ref, local_ref, bias_ref, *refs):
    *far_refs, hidden_ref = refs
    rows, width, channels = high_ref.shape
    block = width + TAIL
    count = mixed_ref.shape[0]
    depth = trig_ref.shape[1]
    local = local_ref[...]
    left, right = side_columns(chips, per, rows, got_ref, far_refs)
    place = lax.broadcasted_iota(jnp.int32, (TAIL, channels), 0)
    first = 6 * count
    lane = lax.broadcasted_iota(jnp.int32, (rows, depth), 1)
    mine = lane == first + lax.broadcasted_iota(jnp.int32, (rows, depth), 0)
    dry = [
        jnp.sum(jnp.where(mine, 1.0 - side[:, channels : channels + 1], 0.0), 0, keepdims=True)
        for side in (left, right)
    ]
    tail_place = lax.broadcasted_iota(jnp.int32, (TAIL, depth), 0)
    tail_lane = lax.broadcasted_iota(jnp.int32, (TAIL, depth), 1)
    is_land = (tail_lane >= first) & (tail_lane < first + rows)
    end = trig_ref[width:, :].astype(F32)
    end = jnp.where(is_land & (tail_place == TAIL - 1), dry[0], end)
    end = jnp.where(is_land & (tail_place == 0), dry[1], end)
    trig = jnp.concatenate([trig_ref[:width, :], end.astype(BF16)], 0)
    bias = bias_rows(bias_ref)
    select = lax.broadcasted_iota(jnp.int32, (rows, channels), 0)
    for i in range(0, rows, 2):
        parts, mixed, cuts = [], [], []
        for r in (i, i + 1):
            side = jnp.where(
                place == TAIL - 1, left[r : r + 1, :channels], jnp.where(place == 0, right[r : r + 1, :channels], 0.0)
            )
            high, low = split(side)
            parts.append((jnp.concatenate([high_ref[r], high], 0), jnp.concatenate([low_ref[r], low], 0)))
            mixed.append(jnp.concatenate([mixed_ref[:, r, :channels], mixed_ref[:, r, channels:]], 0))
            cuts.append(jnp.where(select == r, DRY, 0.0))
        pair = hidden_pair(parts, mixed, cuts, trig, local, bias, channels)
        for r in range(2):
            hidden_ref[(i + r) * block : (i + r + 1) * block, :] = pair[r]


def columns(t, channels, keep):
    west = pltpu.roll(t[:, :channels], 1, 0)
    east = pltpu.roll(t[:, 2 * channels :], t.shape[0] - 1, 0)
    return (west + t[:, channels : 2 * channels] + east)[:keep]


def product(parts, weights, channels):
    y = dot(jnp.concatenate(split(jnp.concatenate(parts, 0)), 1), weights)
    return y[:, : 3 * channels] + y[:, 3 * channels :]


def inner_kernel(groups, hidden_ref, ocean_ref, bias_ref, filter_ref, out_ref):
    _, width = ocean_ref.shape
    channels = hidden_ref.shape[1]
    block = width + TAIL
    wet = ocean_ref[...].astype(F32).T

    def rows_of(first, count):
        return [hidden_ref[(first - 1 + k) * block : (first + k) * block, :] for k in range(count)]

    def write(sums, firsts):
        for g, first in enumerate(firsts):
            for r, t in enumerate(sums):
                t = columns(t[g * block : (g + 1) * block], channels, width)
                row = first + r
                out_ref[row - 1] = (t + bias_ref[...]) * wet[:, row : row + 1]

    quads, pairs = groups
    if quads:
        terms = [[] for _ in range(6)]
        for first in quads:
            d = rows_of(first, 6)
            a, b = d[4] - 4.0 * d[2], d[3] - 4.0 * d[1]
            p, q = d[4] - d[2], 2.0 * (d[3] - d[1])
            for k, term in enumerate(
                (4.0 * d[0] - 5.0 * d[2] + d[4], a + b, a - b, p + q, p - q, 4.0 * d[1] - 5.0 * d[3] + d[5])
            ):
                terms[k].append(term)
        m = [product(terms[k], filter_ref[index], channels) for k, index in enumerate((5, 6, 7, 8, 9, 3))]
        sum1, dif1, sum2, dif2 = m[1] + m[2], m[1] - m[2], m[3] + m[4], m[3] - m[4]
        write((m[0] + sum1 + sum2, dif1 + 2.0 * dif2, sum1 + 4.0 * sum2, dif1 + 8.0 * dif2 + m[5]), quads)
    if pairs:
        terms = [[] for _ in range(4)]
        for first in pairs:
            d = rows_of(first, 4)
            for k, term in enumerate((d[0] - d[2], d[1] + d[2], d[2] - d[1], d[1] - d[3])):
                terms[k].append(term)
        m = [product(terms[k], filter_ref[k], channels) for k in range(4)]
        write((m[0] + m[1] + m[2], m[1] - m[2] - m[3]), pairs)


def outer_kernel(
    bands, hidden_ref, early_first, early_second, late_first, late_second, trig_ref, local_ref, layer_ref,
    ocean_ref, bias_ref, filter_ref, inner_ref, out_ref, buf_ref, sem_ref,
):
    rows, width = ocean_ref.shape
    channels = local_ref.shape[0]
    block = width + TAIL
    middle = pltpu.make_async_copy(inner_ref, out_ref.at[pl.ds(1, rows - 2)], sem_ref.at[2])
    middle.start()
    wet = ocean_ref[...].astype(F32).T
    layer = bias_rows(layer_ref)
    no_cut = jnp.zeros((rows, channels), F32)
    place = lax.broadcasted_iota(jnp.int32, (TAIL, channels), 0)

    def neighbour(early, late):
        count = late.shape[0] - 8
        left, right = late[count : count + 1, :], late[count + 1 : count + 2, :]

        def tail(lanes):
            return jnp.where(place == TAIL - 1, left[:, lanes], jnp.where(place == 0, right[:, lanes], 0.0))

        flags = early[width:, :].T
        pieces = [jnp.broadcast_to(flags[:, k : k + 1], (channels, channels)) for k in range(width // channels)]
        mask = jnp.concatenate(pieces + [tail(slice(channels, None))], 0)
        x = jnp.concatenate([early[:width, :], tail(slice(0, channels))], 0)
        mixed = jnp.concatenate([late[:count, :channels], late[:count, channels:]], 0)
        return mask, split(x), mixed

    band = lax.axis_index("lat")
    even = lax.rem(band, 2) == 0
    masks, parts, mixed = zip(neighbour(early_first, late_first), neighbour(early_second, late_second))
    pair = hidden_pair(parts, mixed, (no_cut, no_cut), trig_ref[...], local_ref[...], layer, channels)
    one, two = (mask * y for mask, y in zip(masks, pair))
    above = jnp.where(band == 0, 0.0, jnp.where(even, two, one))
    below = jnp.where(band == bands - 1, 0.0, jnp.where(even, one, two))

    def at(row):
        return hidden_ref[row * block : (row + 1) * block, :]

    z = product([at(0), at(rows - 1)], filter_ref[4], channels)
    z = z + product([at(1), below], filter_ref[3], channels)
    z = z + product([above, at(rows - 2)], filter_ref[0], channels)
    copies = [middle]
    for r, row in enumerate((0, rows - 1)):
        t = columns(z[r * block : (r + 1) * block], channels, width)
        buf_ref[r] = (t + bias_ref[...]) * wet[:, row : row + 1]
        copy = pltpu.make_async_copy(buf_ref.at[pl.ds(r, 1)], out_ref.at[pl.ds(row, 1)], sem_ref.at[r])
        copy.start()
        copies.append(copy)
    for copy in copies:
        copy.wait()


def vmem():
    return pl.BlockSpec(memory_space=pltpu.VMEM)


def struct(shape, dtype=F32):
    return jax.ShapeDtypeStruct(shape, dtype)


def params(mib):
    return pltpu.CompilerParams(vmem_limit_bytes=mib * MIB)


def per_device(
    field, ocean, modes, spectral_weight, local_weight, layer_bias, conv_weight, conv_bias
):
    rows, width, channels = field.shape
    devices = lax.axis_size("lon")
    chips = devices // 2
    bands = lax.axis_size("lat")
    total_lon = width * devices
    total_modes = modes.shape[0]
    per = total_modes // devices
    half = chips * per
    block = width + TAIL
    steps = list(range(1, chips))
    wide = 2 * channels
    chunks = 2

    give, keep, away, early_first, early_second, high, low = pl.pallas_call(
        functools.partial(forward_kernel, chips, per, total_lon),
        out_shape=(
            struct((half + 1, rows, wide)),
            struct((half, rows, wide)),
            struct((1, rows, wide)),
            struct((width + 8, channels)),
            struct((width + 8, channels)),
            struct((rows, width, channels), BF16),
            struct((rows, width, channels), BF16),
        ),
        in_specs=[pl.BlockSpec(memory_space=pltpu.MemorySpace.HBM)] * 3,
        out_specs=(vmem(),) * 7,
        scratch_shapes=[
            pltpu.SMEM((total_modes,), jnp.int32),
            pltpu.VMEM((rows, width, channels), F32),
            pltpu.VMEM((rows, width), jnp.int32),
            pltpu.SemaphoreType.DMA((2,)),
            pltpu.SemaphoreType.DMA((chunks,)),
        ],
        compiler_params=params(16),
        name="forward",
    )(*[pltpu.with_memory_space_constraint(x, pltpu.MemorySpace.HBM) for x in (modes, field, ocean)])
    give = give.reshape((half + 1) * rows, wide)
    keep = keep.reshape(half * rows, wide)
    away = away.reshape(rows, wide)

    depth = -(-(6 * total_modes + rows + 8) // LANES) * LANES
    trig, local, mix = pl.pallas_call(
        functools.partial(prepare_kernel, chips, per, total_lon),
        out_shape=(
            struct((block, depth), BF16),
            struct((channels, 2 * channels), BF16),
            struct((per * wide, 2 * wide), BF16),
        ),
        in_specs=[vmem()] * 4,
        out_specs=(vmem(),) * 3,
        compiler_params=params(16),
        name="prepare",
    )(modes.reshape(1, total_modes), local_weight, spectral_weight, ocean)
    filters = pl.pallas_call(
        filter_kernel,
        out_shape=struct((10, 2 * channels, 6 * channels), BF16),
        in_specs=[vmem()],
        out_specs=vmem(),
        compiler_params=params(16),
        name="filters",
    )(conv_weight)

    got = lax.ppermute(give, "lon", pair_moves(chips))
    summed = keep + got[: half * rows]
    size = per * rows
    parts = {}
    for d in steps:
        send = summed[d * size : (d + 1) * size]
        if flip_of(d):
            send = jnp.concatenate([send, away])
        parts[d] = lax.ppermute(send, "lon", chip_moves(d, chips, flip_of(d)))
    crossed = [parts[d] for d in steps if flip_of(d)]
    evens = [(i, i + 1) for i in range(0, bands - 1, 2)]
    odds = [(i, i + 1) for i in range(1, bands - 1, 2)]
    if bands % 2 == 0 and bands > 2:
        odds.append((0, bands - 1))
    evens, odds = ([(a, b) for a, b in moves] + [(b, a) for a, b in moves] for moves in (evens, odds))
    early_first = lax.ppermute(early_first, "lat", evens)
    early_second = lax.ppermute(early_second, "lat", odds)

    own_mixed = pl.pallas_call(
        functools.partial(mix_kernel, per, rows),
        out_shape=struct((size, wide)),
        in_specs=[vmem()] * (len(steps) + 2),
        out_specs=vmem(),
        compiler_params=params(8),
        name="mix",
    )(summed, *[parts[d] for d in steps], mix)
    gathered = [own_mixed]
    for d in steps:
        gathered.append(lax.ppermute(own_mixed, "lon", chip_moves(d, chips, 0)))
    gathered = jnp.concatenate(gathered)
    other = lax.ppermute(gathered, "lon", pair_moves(chips))
    mixed = jnp.concatenate([gathered, other]).reshape(total_modes, rows, wide)

    late = struct((total_modes + 8, wide))
    late_first, late_second = pl.pallas_call(
        functools.partial(edges_kernel, chips, per),
        out_shape=(late, late),
        in_specs=[vmem()] * (2 + len(crossed)),
        out_specs=(vmem(),) * 2,
        compiler_params=params(8),
        name="edges",
    )(got, mixed, *crossed)
    late_first = lax.ppermute(late_first, "lat", evens)
    late_second = lax.ppermute(late_second, "lat", odds)
    layer = layer_bias.reshape(1, channels)
    hidden = pl.pallas_call(
        functools.partial(hidden_kernel, chips, per),
        out_shape=struct((rows * block, channels)),
        in_specs=[vmem()] * (7 + len(crossed)),
        out_specs=vmem(),
        compiler_params=params(24),
        cost_estimate=pl.CostEstimate(
            flops=6 * 256 * rows * width * channels, transcendentals=field.size, bytes_accessed=4 * field.size
        ),
        name="hidden",
    )(high, low, got, mixed, trig, local, layer, *crossed)

    bias = conv_bias.reshape(1, channels)
    whole = (rows - 2) // 4 * 4
    groups = (list(range(1, whole, 4)), list(range(1 + whole, rows - 1, 2)))
    flops = 2 * 6 * 4 * rows * width * channels * channels
    inner = pl.pallas_call(
        functools.partial(inner_kernel, groups),
        out_shape=struct((rows - 2, width, channels)),
        in_specs=[vmem()] * 4,
        out_specs=vmem(),
        compiler_params=params(24),
        cost_estimate=pl.CostEstimate(flops=flops, transcendentals=0, bytes_accessed=4 * field.size),
        name="inner",
    )(hidden, ocean, bias, filters)
    return pl.pallas_call(
        functools.partial(outer_kernel, bands),
        out_shape=struct((rows, width, channels)),
        in_specs=[vmem()] * 12,
        out_specs=pl.BlockSpec(memory_space=pl.ANY),
        scratch_shapes=[
            pltpu.VMEM((2, width, channels), F32),
            pltpu.SemaphoreType.DMA((3,)),
        ],
        compiler_params=params(24),
        name="outer",
    )(
        hidden, early_first, early_second, late_first, late_second, trig, local, layer, ocean, bias, filters, inner
    )


def solution(mesh):
    in_specs = (
        P("lat", "lon", None),
        P("lat", "lon"),
        P(),
        P("lon", None, None, None),
        P(),
        P(),
        P(),
        P(),
    )
    out_specs = P("lat", "lon", None)
    return jax.shard_map(
        per_device, mesh=mesh, in_specs=in_specs, out_specs=out_specs, check_vma=False
    )
```
